32 devices in a mesh: section: 4 (over y, x), owner: 8 (over z, core).
Axes of the slice: x: 2, y: 2, z: 4, core: 2. Of those that a mesh axis runs over, the one named last changes fastest.
Arguments:
- weights: bfloat16 [4, 1024, 1024], P('section'), may hold values from -0.1875 to 0.1875
- inputs: bfloat16 [4, 4, 2048, 1024], P('section', None, 'owner'), may hold values from -6 to 6
- preact: bfloat16 [4, 4, 2048, 1024], P('section', None, 'owner'), may hold values from -6 to 6
- cotangent: bfloat16 [4, 2048, 1024], P(None, 'owner'), may hold values from -6 to 6
- embeddings: bfloat16 [4, 2048, 32, 128], P(None, ('owner', 'section')), may hold values from -6 to 6
- row_ids: int32 [4, 2048, 32], P(None, ('owner', 'section')), may hold values from 0 to 511
Outputs:
- weight_grad: float32 [4, 1024, 1024], P('section', 'owner')
- table_grad: float32 [32, 512, 128], P('owner', 'section')
The draws below stay inside these ranges and needn't reach their ends.
All inputs are finite; a program needn't handle non-finite values.
Results may differ from the reference program's by a relative error of at most 0.0064.
Values may be sent and summed in bfloat16 or wider, within the bound.
A program may use at most 128 MiB of HBM per device.

```python
import math
import jax
import jax.numpy as jnp
import numpy as np
from jax import lax

F = 32
E = 128
H = 1024
MICRO = 4
TROWS = 512
LAYERS = 4
SLOTS = 32
ROWS = 512
BATCH = 2048


def with_ends(values, own_key, low, high):
    longest = values.shape.index(max(values.shape))
    spots = []
    for shift in (0, 1):
        where = [jax.random.randint(jax.random.fold_in(own_key, axis), (), 0, length) for axis, length in enumerate(values.shape)]
        where[longest] = (where[longest] + shift) % values.shape[longest]
        spots.append(tuple(where))
    return values.at[spots[0]].set(low).at[spots[1]].set(high)


def spiked(drawn, key, source, target, blocks, factor):
    def block_of(dim):
        return (jnp.arange(drawn.shape[dim]) // (drawn.shape[dim] // blocks)).reshape((-1,) + (1,) * (drawn.ndim - 1 - dim))

    near = jax.random.permutation(key, blocks)[block_of(target)]
    other_side = (block_of(target) + blocks // 2) % blocks
    return jnp.where((block_of(source) == near) | (block_of(source) == other_side), factor * drawn, drawn)


def shard_levels(key, extent, split, least, top_value):
    loudness = 1.0
    for dim, shards_of in split:
        draws = jax.random.uniform(jax.random.fold_in(jax.random.fold_in(key, 6), dim), (shards_of,), jnp.float32, least / len(split), top_value / len(split))
        loudness = loudness * jnp.repeat(jnp.exp(draws), extent[dim] // shards_of).reshape((-1,) + (1,) * (len(extent) - 1 - dim))
    return loudness


def rank_bounds(amount, skew):
    weights = [(1 << 20) // math.isqrt(standing ** skew) + 1 for standing in range(1, amount + 1)]
    deviation = 1 + sum(weights) // (1 << 30)
    return np.cumsum(np.array([max(1, weight // deviation) for weight in weights]))


def skewed_ids(stream_key, dims, number_of, skew):
    listing = rank_bounds(number_of, skew)
    ticket = jax.random.randint(jax.random.fold_in(stream_key, 1), dims, 0, int(listing[number_of - 1]))
    grade = jnp.searchsorted(jnp.asarray(listing, jnp.int32), ticket, side="right")
    return jax.random.permutation(jax.random.fold_in(stream_key, 2), number_of)[grade].astype(jnp.int32)


def gaussian(key, extent, width, limit, pieces=(), held_as=jnp.bfloat16):
    drawn = width * jax.random.normal(key, extent, jnp.float32)
    if pieces:
        drawn = drawn * shard_levels(key, extent, pieces, -0.22, 0.18)
    return jnp.clip(drawn, -limit, limit).astype(held_as)


def gaussian_with(rng, extent, spread, limit, pieces, heavy, kind=jnp.bfloat16):
    values = spread * jax.random.normal(rng, extent, jnp.float32)
    if pieces:
        values = values * shard_levels(rng, extent, pieces, -0.22, 0.18)
    return jnp.clip(spiked(values, jax.random.fold_in(rng, 3), *heavy), -limit, limit).astype(kind)


def setup_inputs(seed: int = 0) -> dict:
    arg_keys = jax.random.split(jax.random.key(seed), 7)
    return {
        "weights": gaussian(arg_keys[0], (LAYERS, H, H), H ** -0.5, 0.1875, ((0, 4),)),
        "inputs": gaussian_with(arg_keys[1], (LAYERS, MICRO, BATCH, H), 1.0, 6.0, ((0, 4), (2, 8)), (2, 3, 8, 2.0)),
        "preact": gaussian(arg_keys[2], (LAYERS, MICRO, BATCH, H), 1.0, 6.0, ((0, 4), (2, 8))),
        "cotangent": gaussian(arg_keys[3], (MICRO, BATCH, H), 1.0, 6.0, ((1, 8),)),
        "embeddings": gaussian(arg_keys[4], (MICRO, BATCH, F, E), 1.0, 6.0, ((1, 32),)),
        "row_ids": with_ends(skewed_ids(arg_keys[5], (MICRO, BATCH, F), ROWS, 2), jax.random.fold_in(arg_keys[5], 3), 0, ROWS - 1).astype(jnp.int32),
    }


def reference(weights, inputs, preact, cotangent, embeddings, row_ids):
    highest = lax.Precision.HIGHEST
    micro_count, sample_rows, hidden = cotangent.shape
    features = embeddings.shape[2]
    emb_width = embeddings.shape[3]
    grad_scale = 1.0 / math.sqrt(micro_count * sample_rows)
    upstream = cotangent
    layer_grads = []
    for layer_index in range(LAYERS - 1, -1, -1):
        slope = jnp.where(preact[layer_index] > 0, upstream, jnp.zeros_like(upstream))
        slope = slope.reshape(micro_count * sample_rows, hidden)
        flat_in = inputs[layer_index].reshape(micro_count * sample_rows, hidden)
        layer_grads.append(jnp.dot(flat_in.T.astype(jnp.float32), slope.astype(jnp.float32), precision=highest) * grad_scale)
        upstream = jnp.dot(slope.astype(jnp.float32), weights[layer_index].T.astype(jnp.float32), precision=highest)
        upstream = upstream.astype(jnp.bfloat16).reshape(micro_count, sample_rows, hidden)
    weight_grad = jnp.stack(layer_grads[::-1])

    def feature_grads(members):
        flat_grad, embedded = members
        square = flat_grad.reshape(sample_rows, features, features).astype(jnp.float32)
        emb32 = embedded.astype(jnp.float32)
        direct = jnp.einsum('qfg,qge->qfe', square, emb32, precision=highest)
        swapped = jnp.einsum('qgf,qge->qfe', square, emb32, precision=highest)
        return (direct + swapped).astype(jnp.bfloat16)
    grads_all = lax.map(feature_grads, (upstream, embeddings))
    flat_grads = grads_all.reshape(micro_count * sample_rows, features, emb_width)
    flat_ids = row_ids.reshape(micro_count * sample_rows, features)

    def one_table(feature_index):
        column = lax.dynamic_index_in_dim(flat_grads, feature_index, 1, False).astype(jnp.float32)
        row_index = lax.dynamic_index_in_dim(flat_ids, feature_index, 1, False)
        return jax.ops.segment_sum(column, row_index, num_segments=ROWS)
    tables = lax.map(one_table, jnp.arange(features, dtype=jnp.int32))
    table_grad = (tables * grad_scale).reshape(SLOTS, TROWS, emb_width)
    return (weight_grad, table_grad)
```

```python
import functools
import math

import jax
import jax.numpy as jnp
from jax import lax
from jax.experimental import pallas as pl
from jax.experimental.pallas import tpu as pltpu
from jax.sharding import PartitionSpec as P

TROWS = 512
PIECE = 16
SPAN = 512


def exclusive_or(a, b, bits):
    total = 0
    for k in range(bits):
        total = total + lax.rem(a // (1 << k) + b // (1 << k), 2) * (1 << k)
    return total


def step_kernel(
    dims, w_hbm, pre_hbm, cot_hbm, in_hbm, emb_hbm, ids_ref, wg_ref, table_ref,
    w, pre, cot, inp, emb, slope, in_buf, out_buf, portion, square, pairs, outgoing, arrived,
    places, ids, acc, wsend, wrecv, tacc, tsend, trecv,
    w_sem, pre_sem, cot_sem, inp_sem, emb_sem, out_sem, in_sem, portion_sem, send_sem, recv_sem,
    ids_send, ids_recv, wsend_sem, wrecv_sem, tsend_sem, trecv_sem,
):
    sections, owners, micro_count, quarter, features, width, slots, row_split, grad_scale = dims
    section = lax.axis_index("section")
    owner = lax.axis_index("owner")
    last = sections - 1
    lane_groups = 128 // features
    hidden = w.shape[0]
    per_micro = quarter // PIECE
    chunks = micro_count * per_micro
    chunk_rows = sections * PIECE
    bits = owners.bit_length() - 1
    block = hidden // owners
    share = TROWS // sections

    barrier = pltpu.get_barrier_semaphore()
    for k in range(1, owners):
        pl.semaphore_signal(
            barrier, inc=1, device_id={"owner": lax.rem(owner + k, owners)},
            device_id_type=pl.DeviceIdType.MESH,
        )
    for k in range(1, sections):
        pl.semaphore_signal(
            barrier, inc=1, device_id={"section": lax.rem(section + k, sections)},
            device_id_type=pl.DeviceIdType.MESH,
        )

    def load_w():
        return pltpu.make_async_copy(w_hbm, w, w_sem)

    def load_pre(m):
        return pltpu.make_async_copy(pre_hbm.at[m], pre.at[m], pre_sem.at[m])

    def load_cot(m):
        return pltpu.make_async_copy(cot_hbm.at[m], cot.at[m], cot_sem.at[m])

    def load_inp():
        return pltpu.make_async_copy(in_hbm, inp, inp_sem)

    def load_emb():
        return pltpu.make_async_copy(emb_hbm, emb, emb_sem)

    load_w().start()
    for m in range(micro_count):
        load_pre(m).start()

        @pl.when(section == last)
        def _():
            load_cot(m).start()

    load_emb().start()
    load_inp().start()
    acc[...] = jnp.zeros_like(acc)
    tacc[...] = jnp.zeros_like(tacc)

    def along(c):
        return pltpu.make_async_remote_copy(
            src_ref=out_buf.at[c], dst_ref=in_buf.at[c],
            send_sem=out_sem.at[c], recv_sem=in_sem.at[c],
            device_id={"section": lax.rem(section + last, sections)},
            device_id_type=pl.DeviceIdType.MESH,
        )

    def hand(c, target):
        return pltpu.make_async_remote_copy(
            src_ref=out_buf.at[c, pl.ds(target * PIECE, PIECE)], dst_ref=portion.at[c],
            send_sem=out_sem.at[c], recv_sem=portion_sem.at[c],
            device_id={"section": target},
            device_id_type=pl.DeviceIdType.MESH,
        )

    def landing(m, j, source):
        return arrived.at[m, source, pl.ds(pl.multiple_of(j * PIECE, PIECE), PIECE)]

    def exchange(c, target):
        return pltpu.make_async_remote_copy(
            src_ref=outgoing.at[target, c],
            dst_ref=landing(c // per_micro, lax.rem(c, per_micro), owner),
            send_sem=send_sem.at[target], recv_sem=recv_sem.at[c],
            device_id={"owner": target},
            device_id_type=pl.DeviceIdType.MESH,
        )

    def exchange_own(c):
        return pltpu.make_async_copy(
            outgoing.at[owner, c],
            landing(c // per_micro, lax.rem(c, per_micro), owner), recv_sem.at[c],
        )

    def exchange_ids(target):
        return pltpu.make_async_remote_copy(
            src_ref=ids_ref.at[target], dst_ref=places.at[owner],
            send_sem=ids_send.at[target], recv_sem=ids_recv,
            device_id={"owner": target},
            device_id_type=pl.DeviceIdType.MESH,
        )

    def reduce_copy(d, k):
        return pltpu.make_async_remote_copy(
            src_ref=wsend.at[d], dst_ref=wrecv.at[d],
            send_sem=wsend_sem.at[d], recv_sem=wrecv_sem.at[d],
            device_id={"owner": exclusive_or(owner, 1 << k, bits)},
            device_id_type=pl.DeviceIdType.MESH,
        )

    def share_copy(target):
        return pltpu.make_async_remote_copy(
            src_ref=tsend.at[target], dst_ref=trecv.at[section],
            send_sem=tsend_sem.at[target], recv_sem=trecv_sem.at[section],
            device_id={"section": target},
            device_id_type=pl.DeviceIdType.MESH,
        )

    def chain(c):
        m, j = c // per_micro, lax.rem(c, per_micro)
        rows = pl.ds(pl.multiple_of(j * PIECE, PIECE), PIECE)

        @pl.when(j == 0)
        def _():
            load_pre(m).wait()

            @pl.when(section == last)
            def _():
                load_cot(m).wait()

        positive = pre[m, :, rows, :].astype(jnp.float32) > 0

        def masked(incoming):
            grad = incoming.astype(jnp.float32)
            slope[m, :, rows, :] = jnp.where(positive, grad, 0.0).astype(jnp.bfloat16)

        @pl.when(section == last)
        def _():
            masked(cot[m, :, rows, :])

        @pl.when(section < last)
        def _():
            along(c).wait_recv()
            masked(in_buf[c].reshape(sections, PIECE, hidden))

        out_buf[c] = lax.dot_general(
            slope[m, :, rows, :].reshape(chunk_rows, hidden), w[...], (((1,), (1,)), ((), ())),
            preferred_element_type=jnp.float32,
        ).astype(jnp.bfloat16)

        @pl.when(section > 0)
        def _():
            along(c).start()

        @pl.when(section == 0)
        def _():
            for target in range(1, sections):
                hand(c, target).start()
            portion[c] = out_buf[c, :PIECE]

    def pair(c):
        m, j = c // per_micro, lax.rem(c, per_micro)

        @pl.when(section > 0)
        def _():
            hand(c, 0).wait_recv()

        for f in range(features):
            group, part = f // lane_groups, f % lane_groups
            piece = portion[c, :, group * 128 : (group + 1) * 128].astype(jnp.float32)
            if part:
                piece = pltpu.roll(piece, 128 - part * features, 1)
            square[pl.ds(f, PIECE, stride=features), :] = piece
        whole = square[...].reshape(PIECE, features, 128)[:, :, :features]
        both = (whole + jnp.swapaxes(whole, 1, 2)).astype(jnp.bfloat16)
        rows = pl.ds(pl.multiple_of(j * PIECE, PIECE), PIECE)
        pairs[...] = lax.dot_general(
            both, emb[m, rows], (((2,), (1,)), ((0,), (0,))),
            preferred_element_type=jnp.float32,
        ).reshape(PIECE * features, width)
        for target in range(owners):
            for slot in range(slots):
                f = (target * slots + slot) // row_split
                outgoing[target, c, :, slot * width : (slot + 1) * width] = pairs[
                    pl.ds(f, PIECE, stride=features), :
                ].astype(jnp.bfloat16)

        def send(k, carry):
            exchange(c, lax.rem(owner + k, owners)).start()
            return carry

        lax.fori_loop(1, owners, send, 0)
        exchange_own(c).start()

    def weigh(m):
        acc[...] += lax.dot_general(
            inp[m], slope[m].reshape(sections * quarter, hidden), (((0,), (0,)), ((), ())),
            preferred_element_type=jnp.float32,
        )

    def block_of(d):
        at = exclusive_or(owner, d, bits) * block
        return pl.ds(pl.multiple_of(at, block), block)

    def send_block(d, k):
        wsend[d] = acc[block_of(d), :].astype(jnp.bfloat16)
        reduce_copy(d, k).start()

    def reduce_stage(k):
        held = owners >> k

        def one(i, carry):
            h = held - 1 - i
            if k > 0:
                d = (1 << (k - 1)) + h * (1 << k)
                reduce_copy(d, k - 1).wait_recv()
                at = block_of(h * (1 << k))
                acc[at, :] = acc[at, :] + wrecv[d].astype(jnp.float32)
            if k < bits:
                @pl.when(lax.rem(h, 2) == 1)
                def _():
                    send_block(h * (1 << k), k)

            return carry

        lax.fori_loop(0, held, one, 0)

    def gather_ids():
        pltpu.make_async_copy(places, places, ids_recv).wait()
        for m in range(micro_count):
            for source in range(owners):
                ids[m, :, source * quarter : (source + 1) * quarter] = places[
                    source, :, m * quarter : (m + 1) * quarter
                ]

    span = min(SPAN, owners * quarter)

    def tabulate(m):
        for j in range(per_micro):
            batch = arrived.at[m, :, pl.ds(j * PIECE, PIECE)]
            pltpu.make_async_copy(batch, batch, recv_sem.at[m * per_micro + j]).wait()

        def one(b, carry):
            sources = span // quarter
            rows = arrived[m, pl.ds(b * sources, sources)].reshape(span, slots * width)
            for slot in range(slots):
                row_block = lax.rem(owner * slots + slot, row_split)
                here = ids[m, slot : slot + 1, pl.ds(pl.multiple_of(b * span, span), span)]
                positions = lax.broadcasted_iota(jnp.int32, (TROWS, span), 0)
                onehot = (positions == here - row_block * TROWS).astype(jnp.float32)
                tacc[slot] += lax.dot_general(
                    onehot.astype(jnp.bfloat16), rows[:, slot * width : (slot + 1) * width],
                    (((1,), (0,)), ((), ())), preferred_element_type=jnp.float32,
                )
            return carry

        lax.fori_loop(0, owners * quarter // span, one, 0)

    def share_tables():
        for target in range(sections):
            @pl.when(section != target)
            def _():
                tsend[target] = tacc[:, target * share : (target + 1) * share, :].astype(jnp.bfloat16)
                share_copy(target).start()

    pl.semaphore_wait(barrier, owners - 1 + sections - 1)

    own_ids = pltpu.make_async_copy(ids_ref.at[owner], places.at[owner], ids_recv)
    own_ids.start()

    def send_ids(k, carry):
        exchange_ids(lax.rem(owner + k, owners)).start()
        return carry

    lax.fori_loop(1, owners, send_ids, 0)
    load_w().wait()

    lag = jnp.where(
        section == last, chunks, jnp.where(section == 0, 0, section * 2 + 2)
    )
    stage_ticks = [chunks - 1, chunks] + [chunks + 6 + 2 * i for i in range(bits - 1)]
    ticks = max(chunks + chunks + 2, stage_ticks[-1] + 1)

    def step(t, carry):
        @pl.when(t < chunks)
        def _():
            chain(t)

            @pl.when(lax.rem(t, per_micro) == per_micro - 1)
            def _():
                m = t // per_micro

                @pl.when(m == 0)
                def _():
                    load_inp().wait()

                weigh(m)

        p = t - lag

        @pl.when((p >= 0) & (p < chunks))
        def _():
            @pl.when(p == 0)
            def _():
                load_emb().wait()

            pair(p)

        for k in range(bits + 1):
            @pl.when(t == stage_ticks[k])
            def _():
                reduce_stage(k)

        @pl.when(p == per_micro)
        def _():
            gather_ids()

        @pl.when((p > per_micro) & (lax.rem(p, per_micro) == 1) & (p < chunks + per_micro))
        def _():
            tabulate(p // per_micro - 1)

        @pl.when(p == chunks + 1)
        def _():
            share_tables()

        return carry

    lax.fori_loop(0, ticks, step, 0)

    wg_ref[...] = acc[block_of(0), :] * grad_scale

    mine = pl.ds(pl.multiple_of(section * share, share), share)
    total = tacc[:, mine, :]
    for k in range(1, sections):
        source = lax.rem(section + k, sections)
        pltpu.make_async_copy(trecv.at[source], trecv.at[source], trecv_sem.at[source]).wait()
        total = total + trecv[source].astype(jnp.float32)
    table_ref[...] = total * grad_scale

    def drain_chain(c, carry):
        @pl.when(section > 0)
        def _():
            along(c).wait_send()

        @pl.when(section == 0)
        def _():
            sent = out_buf.at[c, pl.ds(0, (sections - 1) * PIECE)]
            pltpu.make_async_copy(sent, sent, out_sem.at[c]).wait()

        return carry

    lax.fori_loop(0, chunks, drain_chain, 0)

    def drain_exchange(k, carry):
        target = lax.rem(owner + k, owners)
        sent = outgoing.at[target]
        pltpu.make_async_copy(sent, sent, send_sem.at[target]).wait()
        exchange_ids(target).wait_send()
        reduce_copy(k, 0).wait_send()
        return carry

    lax.fori_loop(1, owners, drain_exchange, 0)
    for k in range(1, sections):
        share_copy(lax.rem(section + k, sections)).wait_send()


def whole_step(layer_w, layer_pre, cotangent, layer_in, embeddings, ids_out, row_split, scale):
    sections = lax.axis_size("section")
    owners = lax.axis_size("owner")
    micro_count, batch_rows, hidden = cotangent.shape
    quarter, features, width = embeddings.shape[1:]
    slots = ids_out.shape[1]
    chunks = micro_count * (quarter // PIECE)
    share = TROWS // sections
    dims = (sections, owners, micro_count, quarter, features, width, slots, row_split, scale)
    vmem = pl.BlockSpec(memory_space=pltpu.VMEM)
    anywhere = pl.BlockSpec(memory_space=pl.ANY)
    narrow, wide, whole = jnp.bfloat16, jnp.float32, jnp.int32
    split = (micro_count, sections, quarter, hidden)
    chunk_shape = (chunks, sections * PIECE, hidden)
    dma = pltpu.SemaphoreType.DMA
    return pl.pallas_call(
        functools.partial(step_kernel, dims),
        out_shape=(
            jax.ShapeDtypeStruct((hidden // owners, hidden), wide),
            jax.ShapeDtypeStruct((slots, share, width), wide),
        ),
        in_specs=[anywhere] * 5 + [vmem],
        out_specs=(vmem, vmem),
        scratch_shapes=[
            pltpu.VMEM((hidden, hidden), narrow),
            pltpu.VMEM(split, narrow),
            pltpu.VMEM(split, narrow),
            pltpu.VMEM((micro_count, batch_rows, hidden), narrow),
            pltpu.VMEM(embeddings.shape, narrow),
            pltpu.VMEM(split, narrow),
            pltpu.VMEM(chunk_shape, narrow),
            pltpu.VMEM(chunk_shape, narrow),
            pltpu.VMEM((chunks, PIECE, hidden), narrow),
            pltpu.VMEM((PIECE * features, 128), wide),
            pltpu.VMEM((PIECE * features, width), wide),
            pltpu.VMEM((owners, chunks, PIECE, slots * width), narrow),
            pltpu.VMEM((micro_count, owners, quarter, slots * width), narrow),
            pltpu.VMEM(ids_out.shape, whole),
            pltpu.VMEM((micro_count, slots, owners * quarter), whole),
            pltpu.VMEM((hidden, hidden), wide),
            pltpu.VMEM((owners, hidden // owners, hidden), narrow),
            pltpu.VMEM((owners, hidden // owners, hidden), narrow),
            pltpu.VMEM((slots, TROWS, width), wide),
            pltpu.VMEM((sections, slots, share, width), narrow),
            pltpu.VMEM((sections, slots, share, width), narrow),
            dma(()),
            dma((micro_count,)),
            dma((micro_count,)),
            dma(()),
            dma(()),
            dma((chunks,)),
            dma((chunks,)),
            dma((chunks,)),
            dma((owners,)),
            dma((chunks,)),
            dma((owners,)),
            dma(()),
            dma((owners,)),
            dma((owners,)),
            dma((sections,)),
            dma((sections,)),
        ],
        compiler_params=pltpu.CompilerParams(
            collective_id=0, has_side_effects=True, vmem_limit_bytes=56 * 1024 * 1024
        ),
    )(
        layer_w, layer_pre.reshape(split), cotangent.reshape(split), layer_in, embeddings, ids_out
    )


def per_device(weights, inputs, preact, cotangent, embeddings, row_ids):
    owners = lax.axis_size("owner")
    micro_count, batch_rows, hidden = cotangent.shape
    quarter, features, width = embeddings.shape[1:]
    row_split = max(1, owners // features)
    slots = features * row_split // owners
    grad_scale = 1.0 / math.sqrt(micro_count * batch_rows * owners)
    ids_out = jnp.repeat(
        row_ids.reshape(micro_count * quarter, features).T, row_split, axis=0
    ).reshape(owners, slots, micro_count * quarter)
    weight_grad, table_grad = whole_step(
        weights[0], preact[0], cotangent, inputs[0], embeddings, ids_out, row_split, grad_scale
    )
    return (weight_grad[None], table_grad)


def solution(mesh):
    return jax.shard_map(
        per_device,
        mesh=mesh,
        in_specs=(
            P("section", None, None),
            P("section", None, "owner", None),
            P("section", None, "owner", None),
            P(None, "owner", None),
            P(None, ("owner", "section"), None, None),
            P(None, ("owner", "section"), None),
        ),
        out_specs=(P("section", "owner", None), P("owner", "section", None)),
        check_vma=False,
    )
```

```python
import functools
import math

import jax
import jax.numpy as jnp
from jax import lax
from jax.experimental import pallas as pl
from jax.experimental.pallas import tpu as pltpu
from jax.sharding import PartitionSpec as P

TROWS = 512
PIECE = 16
SPAN = 512
GROUP = 2


def exclusive_or(a, b, bits):
    total = 0
    for k in range(bits):
        total = total + lax.rem(a // (1 << k) + b // (1 << k), 2) * (1 << k)
    return total


def step_kernel(
    dims, w_hbm, pre_hbm, cot_hbm, in_hbm, emb_hbm, ids_hbm, wg_ref, table_ref,
    w, wt, pre, cot, inp, emb, raw, slope, in_buf, out_buf, portion, square, pairs, outgoing,
    arrived, mine, places, ids, acc, wsend, wrecv, tacc, tsend, trecv,
    w_sem, pre_sem, cot_sem, inp_sem, emb_sem, raw_sem, out_sem, in_sem, hand_sem, portion_sem,
    send_sem, recv_sem, ids_send, ids_recv, wsend_sem, wrecv_sem, tsend_sem, trecv_sem,
):
    sections, owners, micro_count, quarter, features, width, slots, row_split = dims
    section = lax.axis_index("section")
    owner = lax.axis_index("owner")
    last = sections - 1
    lane_groups = 128 // features
    hidden = w.shape[0]
    per_micro = quarter // PIECE
    chunks = micro_count * per_micro
    subs = sections // GROUP
    bits = owners.bit_length() - 1
    block = hidden // owners
    share = TROWS // sections

    barrier = pltpu.get_barrier_semaphore()
    for k in range(1, sections):
        pl.semaphore_signal(
            barrier, inc=1, device_id={"section": lax.rem(section + k, sections)},
            device_id_type=pl.DeviceIdType.MESH,
        )
    for k in range(1, owners):
        pl.semaphore_signal(
            barrier, inc=1, device_id={"owner": lax.rem(owner + k, owners)},
            device_id_type=pl.DeviceIdType.MESH,
        )

    def load_w():
        return pltpu.make_async_copy(w_hbm, w, w_sem)

    def load_pre(m):
        return pltpu.make_async_copy(pre_hbm.at[m], pre.at[m], pre_sem.at[m])

    def load_cot(m):
        return pltpu.make_async_copy(cot_hbm.at[m], cot.at[m], cot_sem.at[m])

    def load_inp():
        return pltpu.make_async_copy(in_hbm, inp, inp_sem)

    def load_emb():
        return pltpu.make_async_copy(emb_hbm, emb, emb_sem)

    def load_raw():
        return pltpu.make_async_copy(ids_hbm, raw, raw_sem)

    load_w().start()
    for m in range(micro_count):
        load_pre(m).start()

        @pl.when(section == last)
        def _():
            load_cot(m).start()

    load_raw().start()
    load_emb().start()
    load_inp().start()

    def rows_of(j):
        return pl.ds(pl.multiple_of(j * PIECE, PIECE), PIECE)

    def place(u):
        c = u // subs
        base = (subs - 1 - lax.rem(u, subs)) * GROUP
        return c // per_micro, pl.ds(base, GROUP), rows_of(lax.rem(c, per_micro))

    def along(u):
        at = place(u)
        return pltpu.make_async_remote_copy(
            src_ref=out_buf.at[at], dst_ref=in_buf.at[at],
            send_sem=out_sem.at[u], recv_sem=in_sem.at[u],
            device_id={"section": lax.rem(section + last, sections)},
            device_id_type=pl.DeviceIdType.MESH,
        )

    def hand(c, target):
        return pltpu.make_async_remote_copy(
            src_ref=out_buf.at[c // per_micro, target, rows_of(lax.rem(c, per_micro))],
            dst_ref=portion.at[c],
            send_sem=hand_sem.at[c], recv_sem=portion_sem.at[c],
            device_id={"section": target},
            device_id_type=pl.DeviceIdType.MESH,
        )

    def landing(c):
        return arrived.at[c // per_micro, owner, rows_of(lax.rem(c, per_micro))]

    def exchange(c, target):
        return pltpu.make_async_remote_copy(
            src_ref=outgoing.at[target, c], dst_ref=landing(c),
            send_sem=send_sem.at[target], recv_sem=recv_sem.at[c],
            device_id={"owner": target},
            device_id_type=pl.DeviceIdType.MESH,
        )

    def exchange_ids(target):
        return pltpu.make_async_remote_copy(
            src_ref=mine.at[target], dst_ref=places.at[owner],
            send_sem=ids_send.at[target], recv_sem=ids_recv,
            device_id={"owner": target},
            device_id_type=pl.DeviceIdType.MESH,
        )

    def reduce_copy(d, k):
        return pltpu.make_async_remote_copy(
            src_ref=wsend.at[d], dst_ref=wrecv.at[d],
            send_sem=wsend_sem.at[d], recv_sem=wrecv_sem.at[d],
            device_id={"owner": exclusive_or(owner, 1 << k, bits)},
            device_id_type=pl.DeviceIdType.MESH,
        )

    def share_copy(target):
        return pltpu.make_async_remote_copy(
            src_ref=tsend.at[target], dst_ref=trecv.at[section],
            send_sem=tsend_sem.at[target], recv_sem=trecv_sem.at[section],
            device_id={"section": target},
            device_id_type=pl.DeviceIdType.MESH,
        )

    def head(m):
        load_pre(m).wait()
        load_cot(m).wait()
        positive = pre[m].astype(jnp.float32) > 0
        slope[m] = jnp.where(positive, cot[m].astype(jnp.float32), 0.0).astype(jnp.bfloat16)
        out_buf[m] = lax.dot_general(
            slope[m].reshape(sections * quarter, hidden), w[...], (((1,), (1,)), ((), ())),
            preferred_element_type=jnp.float32,
        ).astype(jnp.bfloat16).reshape(sections, quarter, hidden)

        def send(i, carry):
            along(m * per_micro * subs + i).start()
            return carry

        lax.fori_loop(0, per_micro * subs, send, 0)

    def chain(c, i):
        u = c * subs + i
        m, j = c // per_micro, lax.rem(c, per_micro)
        base = (subs - 1 - i) * GROUP
        at = (m, pl.ds(base, GROUP), rows_of(j))
        positive = pre[at].astype(jnp.float32) > 0
        with jax.named_scope("arrive"):
            along(u).wait_recv()
        grad = in_buf[at].astype(jnp.float32)
        slope[at] = jnp.where(positive, grad, 0.0).astype(jnp.bfloat16)
        out_buf[at] = lax.dot_general(
            slope[at].reshape(GROUP * PIECE, hidden), wt[...], (((1,), (0,)), ((), ())),
            preferred_element_type=jnp.float32,
        ).astype(jnp.bfloat16).reshape(GROUP, PIECE, hidden)

        @pl.when(section > 0)
        def _():
            along(u).start()

        @pl.when(section == 0)
        def _():
            for target in range(base, base + GROUP):
                if target == 0:
                    portion[c] = out_buf[m, 0, rows_of(j)]
                else:
                    hand(c, target).start()

    def pair(c):
        m, j = c // per_micro, lax.rem(c, per_micro)

        @pl.when(section > 0)
        def _():
            with jax.named_scope("handed"):
                hand(c, 0).wait_recv()

        for f in range(features):
            group, part = f // lane_groups, f % lane_groups
            piece = portion[c, :, group * 128 : (group + 1) * 128].astype(jnp.float32)
            if part:
                piece = pltpu.roll(piece, 128 - part * features, 1)
            square[pl.ds(f, PIECE, stride=features), :] = piece
        whole = square[...].reshape(PIECE, features, 128)[:, :, :features]
        both = (whole + jnp.swapaxes(whole, 1, 2)).astype(jnp.bfloat16)
        pairs[...] = lax.dot_general(
            both, emb[m, rows_of(j)], (((2,), (1,)), ((0,), (0,))),
            preferred_element_type=jnp.float32,
        ).reshape(PIECE * features, width)
        for target in range(owners):
            for slot in range(slots):
                f = (target * slots + slot) // row_split
                outgoing[target, c, :, slot * width : (slot + 1) * width] = pairs[
                    pl.ds(f, PIECE, stride=features), :
                ].astype(jnp.bfloat16)

        def send(k, carry):
            exchange(c, lax.rem(owner + k, owners)).start()
            return carry

        lax.fori_loop(1, owners, send, 0)
        pltpu.make_async_copy(outgoing.at[owner, c], landing(c), recv_sem.at[c]).start()

    def weigh(m):
        def product():
            return lax.dot_general(
                inp[m], slope[m].reshape(sections * quarter, hidden), (((0,), (0,)), ((), ())),
                preferred_element_type=jnp.float32,
            )

        @pl.when(m == 0)
        def _():
            load_inp().wait()
            acc[...] = product()

        @pl.when(m > 0)
        def _():
            acc[...] += product()

    def block_of(d):
        at = exclusive_or(owner, d, bits) * block
        return pl.ds(pl.multiple_of(at, block), block)

    def reduce_stage(k):
        held = owners >> k

        def one(i, carry):
            h = held - 1 - i
            if k > 0:
                d = (1 << (k - 1)) + h * (1 << k)
                reduce_copy(d, k - 1).wait_recv()
                at = block_of(h * (1 << k))
                acc[at, :] = acc[at, :] + wrecv[d].astype(jnp.float32)
            if k < bits:
                @pl.when(lax.rem(h, 2) == 1)
                def _():
                    d = h * (1 << k)
                    wsend[d] = acc[block_of(d), :].astype(jnp.bfloat16)
                    reduce_copy(d, k).start()

            return carry

        with jax.named_scope(f"reduce{k}"):
            lax.fori_loop(0, held, one, 0)

    def send_ids():
        load_raw().wait()
        for target in range(owners):
            for slot in range(slots):
                f = (target * slots + slot) // row_split
                mine[target, :, slot : slot + 1, :] = raw[:, f : f + 1, :]
        pltpu.make_async_copy(mine.at[owner], places.at[owner], ids_recv).start()

        def send(k, carry):
            exchange_ids(lax.rem(owner + k, owners)).start()
            return carry

        lax.fori_loop(1, owners, send, 0)

    def gather_ids():
        pltpu.make_async_copy(places, places, ids_recv).wait()
        for m in range(micro_count):
            for source in range(owners):
                ids[m, :, source * quarter : (source + 1) * quarter] = places[
                    source, m
                ]
        tacc[...] = jnp.zeros_like(tacc)

    span = min(SPAN, owners * quarter)

    def tabulate(m):
        for j in range(per_micro):
            batch = arrived.at[m, :, pl.ds(j * PIECE, PIECE)]
            pltpu.make_async_copy(batch, batch, recv_sem.at[m * per_micro + j]).wait()

        def one(b, carry):
            sources = span // quarter
            rows = arrived[m, pl.ds(b * sources, sources)].reshape(span, slots * width)
            for slot in range(slots):
                row_block = lax.rem(owner * slots + slot, row_split)
                here = ids[m, slot : slot + 1, pl.ds(pl.multiple_of(b * span, span), span)]
                positions = lax.broadcasted_iota(jnp.int32, (TROWS, span), 0)
                onehot = (positions == here - row_block * TROWS).astype(jnp.float32)
                tacc[slot] += lax.dot_general(
                    onehot.astype(jnp.bfloat16), rows[:, slot * width : (slot + 1) * width],
                    (((1,), (0,)), ((), ())), preferred_element_type=jnp.float32,
                )
            return carry

        with jax.named_scope("tabulate"):
            lax.fori_loop(0, owners * quarter // span, one, 0)

    def share_tables():
        for target in range(sections):
            @pl.when(section != target)
            def _():
                tsend[target] = tacc[:, target * share : (target + 1) * share, :].astype(jnp.bfloat16)
                share_copy(target).start()

    with jax.named_scope("entry"):
        pl.semaphore_wait(barrier, owners - 1 + sections - 1)

    load_w().wait()

    @pl.when(section == last)
    def _():
        def first(m, carry):
            with jax.named_scope("head"):
                head(m)
            return carry

        def second(m, carry):
            with jax.named_scope("weigh"):
                weigh(m)
            return carry

        lax.fori_loop(0, micro_count, first, 0)
        lax.fori_loop(0, micro_count, second, 0)
        reduce_stage(0)
        send_ids()
        reduce_stage(1)

    @pl.when(section < last)
    def _():
        with jax.named_scope("turn"):
            wt[...] = w[...].T
        send_ids()
        for m in range(micro_count):
            load_pre(m).wait()

    lag = jnp.where((section == last) | (section == 0), 0, section * 2 + 1)
    most = last * 2 - 1

    def step(t, carry):
        @pl.when((section < last) & (t < chunks))
        def _():
            for i in range(subs):
                with jax.named_scope("chain"):
                    chain(t, i)

            @pl.when(lax.rem(t, per_micro) == per_micro - 1)
            def _():
                with jax.named_scope("weigh"):
                    weigh(t // per_micro)

            @pl.when(t == chunks - 1)
            def _():
                reduce_stage(0)

        p = t - lag

        @pl.when((p >= 0) & (p < chunks))
        def _():
            @pl.when(p == 0)
            def _():
                load_emb().wait()

            with jax.named_scope("pair"):
                pair(p)

        @pl.when((section < last) & (t == chunks))
        def _():
            reduce_stage(1)

        for k in range(2, bits + 1):
            @pl.when((section == last) & (t == 5 * (k - 1)))
            def _():
                reduce_stage(k)

        @pl.when(p == per_micro)
        def _():
            with jax.named_scope("ids"):
                gather_ids()

        @pl.when((p >= 2 * per_micro) & (lax.rem(p, per_micro) == 0) & (p < chunks))
        def _():
            tabulate(p // per_micro - 2)

        return carry

    lax.fori_loop(0, chunks + max(most, 5 * bits - chunks, 1), step, 0)

    @pl.when((section > 0) & (section < last))
    def _():
        reduce_stage(2)

    tabulate(micro_count - 2)
    tabulate(micro_count - 1)
    share_tables()

    @pl.when(section == 0)
    def _():
        reduce_stage(2)

    here = pl.ds(pl.multiple_of(section * share, share), share)
    total = tacc[:, here, :]
    with jax.named_scope("shared"):
        for k in range(1, sections):
            source = lax.rem(section + k, sections)
            pltpu.make_async_copy(trecv.at[source], trecv.at[source], trecv_sem.at[source]).wait()
            total = total + trecv[source].astype(jnp.float32)
        table_ref[...] = total

    @pl.when(section < last)
    def _():
        for k in range(3, bits + 1):
            reduce_stage(k)

    wg_ref[...] = acc[block_of(0), :]

    def drain_chain(u, carry):
        along(u).wait_send()
        return carry

    @pl.when(section > 0)
    def _():
        lax.fori_loop(0, chunks * subs, drain_chain, 0)

    def drain_hand(c, carry):
        sent = out_buf.at[c // per_micro, pl.ds(0, last), rows_of(lax.rem(c, per_micro))]
        pltpu.make_async_copy(sent, sent, hand_sem.at[c]).wait()
        return carry

    @pl.when(section == 0)
    def _():
        lax.fori_loop(0, chunks, drain_hand, 0)

    def drain_exchange(k, carry):
        target = lax.rem(owner + k, owners)
        sent = outgoing.at[target]
        pltpu.make_async_copy(sent, sent, send_sem.at[target]).wait()
        exchange_ids(target).wait_send()
        reduce_copy(k, 0).wait_send()
        return carry

    lax.fori_loop(1, owners, drain_exchange, 0)
    for k in range(1, sections):
        share_copy(lax.rem(section + k, sections)).wait_send()


def scale_kernel(grad_scale, wg_ref, table_ref, wg_out, table_out):
    wg_out[...] = wg_ref[...] * grad_scale
    table_out[...] = table_ref[...] * grad_scale


def whole_step(layer_w, layer_pre, cotangent, layer_in, embeddings, row_ids, slots, row_split):
    sections = lax.axis_size("section")
    owners = lax.axis_size("owner")
    micro_count, batch_rows, hidden = cotangent.shape
    quarter, features, width = embeddings.shape[1:]
    chunks = micro_count * (quarter // PIECE)
    share = TROWS // sections
    dims = (sections, owners, micro_count, quarter, features, width, slots, row_split)
    vmem = pl.BlockSpec(memory_space=pltpu.VMEM)
    anywhere = pl.BlockSpec(memory_space=pl.ANY)
    narrow, wide, whole = jnp.bfloat16, jnp.float32, jnp.int32
    split = (micro_count, sections, quarter, hidden)
    dma = pltpu.SemaphoreType.DMA
    return pl.pallas_call(
        functools.partial(step_kernel, dims),
        out_shape=(
            jax.ShapeDtypeStruct((hidden // owners, hidden), wide),
            jax.ShapeDtypeStruct((slots, share, width), wide),
        ),
        in_specs=[anywhere] * 6,
        out_specs=(vmem, vmem),
        scratch_shapes=[
            pltpu.VMEM((hidden, hidden), narrow),
            pltpu.VMEM((hidden, hidden), narrow),
            pltpu.VMEM(split, narrow),
            pltpu.VMEM(split, narrow),
            pltpu.VMEM((micro_count, batch_rows, hidden), narrow),
            pltpu.VMEM(embeddings.shape, narrow),
            pltpu.VMEM((micro_count, features, quarter), whole),
            pltpu.VMEM(split, narrow),
            pltpu.VMEM(split, narrow),
            pltpu.VMEM(split, narrow),
            pltpu.VMEM((chunks, PIECE, hidden), narrow),
            pltpu.VMEM((PIECE * features, 128), wide),
            pltpu.VMEM((PIECE * features, width), wide),
            pltpu.VMEM((owners, chunks, PIECE, slots * width), narrow),
            pltpu.VMEM((micro_count, owners, quarter, slots * width), narrow),
            pltpu.VMEM((owners, micro_count, slots, quarter), whole),
            pltpu.VMEM((owners, micro_count, slots, quarter), whole),
            pltpu.VMEM((micro_count, slots, owners * quarter), whole),
            pltpu.VMEM((hidden, hidden), wide),
            pltpu.VMEM((owners, hidden // owners, hidden), narrow),
            pltpu.VMEM((owners, hidden // owners, hidden), narrow),
            pltpu.VMEM((slots, TROWS, width), wide),
            pltpu.VMEM((sections, slots, share, width), narrow),
            pltpu.VMEM((sections, slots, share, width), narrow),
            dma(()),
            dma((micro_count,)),
            dma((micro_count,)),
            dma(()),
            dma(()),
            dma(()),
            dma((chunks * sections // GROUP,)),
            dma((chunks * sections // GROUP,)),
            dma((chunks,)),
            dma((chunks,)),
            dma((owners,)),
            dma((chunks,)),
            dma((owners,)),
            dma(()),
            dma((owners,)),
            dma((owners,)),
            dma((sections,)),
            dma((sections,)),
        ],
        compiler_params=pltpu.CompilerParams(
            collective_id=0, has_side_effects=True, vmem_limit_bytes=56 * 1024 * 1024
        ),
    )(
        layer_w, layer_pre.reshape(split), cotangent.reshape(split), layer_in, embeddings,
        jnp.swapaxes(row_ids, 1, 2),
    )


def per_device(weights, inputs, preact, cotangent, embeddings, row_ids):
    owners = lax.axis_size("owner")
    micro_count, batch_rows, hidden = cotangent.shape
    features = embeddings.shape[2]
    row_split = max(1, owners // features)
    slots = features * row_split // owners
    grad_scale = 1.0 / math.sqrt(micro_count * batch_rows * owners)
    weight_grad, table_grad = whole_step(
        weights[0], preact[0], cotangent, inputs[0], embeddings, row_ids, slots, row_split
    )
    vmem = pl.BlockSpec(memory_space=pltpu.VMEM)
    weight_grad, table_grad = pl.pallas_call(
        functools.partial(scale_kernel, grad_scale),
        out_shape=(
            jax.ShapeDtypeStruct(weight_grad.shape, jnp.float32),
            jax.ShapeDtypeStruct(table_grad.shape, jnp.float32),
        ),
        in_specs=[vmem, vmem],
        out_specs=(vmem, vmem),
    )(weight_grad, table_grad)
    return (weight_grad[None], table_grad)


def solution(mesh):
    return jax.shard_map(
        per_device,
        mesh=mesh,
        in_specs=(
            P("section", None, None),
            P("section", None, "owner", None),
            P("section", None, "owner", None),
            P(None, "owner", None),
            P(None, ("owner", "section"), None, None),
            P(None, ("owner", "section"), None),
        ),
        out_specs=(P("section", "owner", None), P("owner", "section", None)),
        check_vma=False,
    )
```

```python
import functools
import math

import jax
import jax.numpy as jnp
from jax import lax
from jax.experimental import pallas as pl
from jax.experimental.pallas import tpu as pltpu
from jax.sharding import PartitionSpec as P

TROWS = 512
PIECE = 16
SPAN = 512
GROUP = 2
PROXY = 4


def exclusive_or(a, b, bits):
    total = 0
    for k in range(bits):
        total = total + lax.rem(a // (1 << k) + b // (1 << k), 2) * (1 << k)
    return total


def step_kernel(
    dims, w_hbm, pre_hbm, cot_hbm, in_hbm, emb_hbm, ids_hbm, wg_ref, table_ref,
    w, wt, pre, cot, inp, emb, raw, slope, in_buf, out_buf, portion, square, pairs, outgoing,
    arrived, near, mine, places, near_places, ids, near_ids, acc, wsend, wrecv, tacc, nacc,
    tsend, trecv, nsend, nrecv,
    w_sem, pre_sem, cot_sem, inp_sem, emb_sem, raw_sem, out_sem, in_sem, hand_sem, portion_sem,
    send_sem, recv_sem, ids_send, ids_recv, near_send, near_ids_send, near_recv, wsend_sem, wrecv_sem,
    tsend_sem, trecv_sem, nsend_sem, nrecv_sem,
):
    sections, owners, micro_count, quarter, features, width, slots, row_split = dims
    section = lax.axis_index("section")
    owner = lax.axis_index("owner")
    last = sections - 1
    lane_groups = 128 // features
    hidden = w.shape[0]
    per_micro = quarter // PIECE
    chunks = micro_count * per_micro
    subs = sections // GROUP
    bits = owners.bit_length() - 1
    block = hidden // owners
    share = TROWS // sections
    half = owners // 2
    kept = slots // PROXY
    direct = slots - kept
    base_owner = owner // half * half
    mirror = lax.rem(owner + half, owners)

    barrier = pltpu.get_barrier_semaphore()
    for k in range(1, sections):
        pl.semaphore_signal(
            barrier, inc=1, device_id={"section": lax.rem(section + k, sections)},
            device_id_type=pl.DeviceIdType.MESH,
        )
    for k in range(1, owners):
        pl.semaphore_signal(
            barrier, inc=1, device_id={"owner": lax.rem(owner + k, owners)},
            device_id_type=pl.DeviceIdType.MESH,
        )

    if kept:
        for k in range(1, sections):
            pl.semaphore_signal(
                barrier, inc=1,
                device_id={"section": lax.rem(section + k, sections), "owner": mirror},
                device_id_type=pl.DeviceIdType.MESH,
            )

    def load_w():
        return pltpu.make_async_copy(w_hbm, w, w_sem)

    def load_pre(m):
        return pltpu.make_async_copy(pre_hbm.at[m], pre.at[m], pre_sem.at[m])

    def load_cot(m):
        return pltpu.make_async_copy(cot_hbm.at[m], cot.at[m], cot_sem.at[m])

    def load_inp():
        return pltpu.make_async_copy(in_hbm, inp, inp_sem)

    def load_emb():
        return pltpu.make_async_copy(emb_hbm, emb, emb_sem)

    def load_raw():
        return pltpu.make_async_copy(ids_hbm, raw, raw_sem)

    load_w().start()
    for m in range(micro_count):
        load_pre(m).start()

        @pl.when(section == last)
        def _():
            load_cot(m).start()

    load_raw().start()
    load_emb().start()
    load_inp().start()

    def rows_of(j):
        return pl.ds(pl.multiple_of(j * PIECE, PIECE), PIECE)

    def place(u):
        c = u // subs
        base = (subs - 1 - lax.rem(u, subs)) * GROUP
        return c // per_micro, pl.ds(base, GROUP), rows_of(lax.rem(c, per_micro))

    def along(u):
        at = place(u)
        return pltpu.make_async_remote_copy(
            src_ref=out_buf.at[at], dst_ref=in_buf.at[at],
            send_sem=out_sem.at[u], recv_sem=in_sem.at[u],
            device_id={"section": lax.rem(section + last, sections)},
            device_id_type=pl.DeviceIdType.MESH,
        )

    def hand(c, target):
        return pltpu.make_async_remote_copy(
            src_ref=out_buf.at[c // per_micro, target, rows_of(lax.rem(c, per_micro))],
            dst_ref=portion.at[c],
            send_sem=hand_sem.at[c], recv_sem=portion_sem.at[c],
            device_id={"section": target},
            device_id_type=pl.DeviceIdType.MESH,
        )

    def lanes(count):
        return pl.ds(0, count * width)

    def landing(c, count):
        return arrived.at[
            c // per_micro, owner, rows_of(lax.rem(c, per_micro)), lanes(count)
        ]

    def near_landing(c):
        return near.at[c // per_micro, owner - base_owner, rows_of(lax.rem(c, per_micro))]

    def held_back(target, c):
        opposite = lax.rem(target + half, owners)
        return outgoing.at[opposite, c, :, pl.ds(direct * width, kept * width)]

    def exchange(c, target, count):
        return pltpu.make_async_remote_copy(
            src_ref=outgoing.at[target, c, :, lanes(count)], dst_ref=landing(c, count),
            send_sem=send_sem.at[target], recv_sem=recv_sem.at[c],
            device_id={"owner": target},
            device_id_type=pl.DeviceIdType.MESH,
        )

    def exchange_near(c, target):
        return pltpu.make_async_remote_copy(
            src_ref=held_back(target, c), dst_ref=near_landing(c),
            send_sem=near_send.at[target], recv_sem=recv_sem.at[c],
            device_id={"owner": target},
            device_id_type=pl.DeviceIdType.MESH,
        )

    def exchange_ids(target):
        return pltpu.make_async_remote_copy(
            src_ref=mine.at[target], dst_ref=places.at[owner],
            send_sem=ids_send.at[target], recv_sem=ids_recv,
            device_id={"owner": target},
            device_id_type=pl.DeviceIdType.MESH,
        )

    def near_ids_copy(target):
        return pltpu.make_async_remote_copy(
            src_ref=mine.at[lax.rem(target + half, owners)],
            dst_ref=near_places.at[owner - base_owner],
            send_sem=near_ids_send.at[target], recv_sem=near_recv,
            device_id={"owner": target},
            device_id_type=pl.DeviceIdType.MESH,
        )

    def reduce_copy(d, k):
        return pltpu.make_async_remote_copy(
            src_ref=wsend.at[d], dst_ref=wrecv.at[d],
            send_sem=wsend_sem.at[d], recv_sem=wrecv_sem.at[d],
            device_id={"owner": exclusive_or(owner, 1 << k, bits)},
            device_id_type=pl.DeviceIdType.MESH,
        )

    def share_copy(target):
        return pltpu.make_async_remote_copy(
            src_ref=tsend.at[target], dst_ref=trecv.at[section],
            send_sem=tsend_sem.at[target], recv_sem=trecv_sem.at[section],
            device_id={"section": target},
            device_id_type=pl.DeviceIdType.MESH,
        )

    def near_share(target):
        return pltpu.make_async_remote_copy(
            src_ref=nsend.at[target], dst_ref=nrecv.at[section],
            send_sem=nsend_sem.at[target], recv_sem=nrecv_sem.at[section],
            device_id={"section": target, "owner": mirror},
            device_id_type=pl.DeviceIdType.MESH,
        )

    def neighbour(k):
        return base_owner + lax.rem(owner - base_owner + k, half)

    def head(m):
        load_pre(m).wait()
        load_cot(m).wait()
        positive = pre[m].astype(jnp.float32) > 0
        slope[m] = jnp.where(positive, cot[m].astype(jnp.float32), 0.0).astype(jnp.bfloat16)
        out_buf[m] = lax.dot_general(
            slope[m].reshape(sections * quarter, hidden), w[...], (((1,), (1,)), ((), ())),
            preferred_element_type=jnp.float32,
        ).astype(jnp.bfloat16).reshape(sections, quarter, hidden)

        def send(i, carry):
            along(m * per_micro * subs + i).start()
            return carry

        lax.fori_loop(0, per_micro * subs, send, 0)

    def chain(c, i):
        u = c * subs + i
        m, j = c // per_micro, lax.rem(c, per_micro)
        base = (subs - 1 - i) * GROUP
        at = (m, pl.ds(base, GROUP), rows_of(j))
        positive = pre[at].astype(jnp.float32) > 0
        with jax.named_scope("arrive"):
            along(u).wait_recv()
        grad = in_buf[at].astype(jnp.float32)
        slope[at] = jnp.where(positive, grad, 0.0).astype(jnp.bfloat16)
        out_buf[at] = lax.dot_general(
            slope[at].reshape(GROUP * PIECE, hidden), wt[...], (((1,), (0,)), ((), ())),
            preferred_element_type=jnp.float32,
        ).astype(jnp.bfloat16).reshape(GROUP, PIECE, hidden)

        @pl.when(section > 0)
        def _():
            along(u).start()

        @pl.when(section == 0)
        def _():
            for target in range(base, base + GROUP):
                if target == 0:
                    portion[c] = out_buf[m, 0, rows_of(j)]
                else:
                    hand(c, target).start()

    def pair(c):
        m, j = c // per_micro, lax.rem(c, per_micro)

        @pl.when(section > 0)
        def _():
            with jax.named_scope("handed"):
                hand(c, 0).wait_recv()

        for f in range(features):
            group, part = f // lane_groups, f % lane_groups
            piece = portion[c, :, group * 128 : (group + 1) * 128].astype(jnp.float32)
            if part:
                piece = pltpu.roll(piece, 128 - part * features, 1)
            square[pl.ds(f, PIECE, stride=features), :] = piece
        whole = square[...].reshape(PIECE, features, 128)[:, :, :features]
        both = (whole + jnp.swapaxes(whole, 1, 2)).astype(jnp.bfloat16)
        pairs[...] = lax.dot_general(
            both, emb[m, rows_of(j)], (((2,), (1,)), ((0,), (0,))),
            preferred_element_type=jnp.float32,
        ).reshape(PIECE * features, width)
        for target in range(owners):
            for slot in range(slots):
                f = (target * slots + slot) // row_split
                outgoing[target, c, :, slot * width : (slot + 1) * width] = pairs[
                    pl.ds(f, PIECE, stride=features), :
                ].astype(jnp.bfloat16)

        def send_far(k, carry):
            exchange(c, lax.rem(neighbour(k) + half, owners), direct).start()
            return carry

        def send_close(k, carry):
            exchange(c, neighbour(k), slots).start()
            if kept:
                exchange_near(c, neighbour(k)).start()
            return carry

        lax.fori_loop(0, half, send_far, 0)
        lax.fori_loop(1, half, send_close, 0)
        pltpu.make_async_copy(outgoing.at[owner, c], landing(c, slots), recv_sem.at[c]).start()
        if kept:
            pltpu.make_async_copy(held_back(owner, c), near_landing(c), recv_sem.at[c]).start()

    def weigh(m):
        def product():
            return lax.dot_general(
                inp[m], slope[m].reshape(sections * quarter, hidden), (((0,), (0,)), ((), ())),
                preferred_element_type=jnp.float32,
            )

        @pl.when(m == 0)
        def _():
            load_inp().wait()
            acc[...] = product()

        @pl.when(m > 0)
        def _():
            acc[...] += product()

    def block_of(d):
        at = exclusive_or(owner, d, bits) * block
        return pl.ds(pl.multiple_of(at, block), block)

    def reduce_stage(k, part=None):
        held = owners >> k
        top = held // 2 if part == 1 else held
        count = held if part is None else held // 2

        def one(i, carry):
            h = top - 1 - i
            if k > 0:
                d = (1 << (k - 1)) + h * (1 << k)
                reduce_copy(d, k - 1).wait_recv()
                at = block_of(h * (1 << k))
                acc[at, :] = acc[at, :] + wrecv[d].astype(jnp.float32)
            if k < bits:
                @pl.when(lax.rem(h, 2) == 1)
                def _():
                    d = h * (1 << k)
                    wsend[d] = acc[block_of(d), :].astype(jnp.bfloat16)
                    reduce_copy(d, k).start()

            return carry

        with jax.named_scope(f"reduce{k}"):
            lax.fori_loop(0, count, one, 0)

    def send_ids():
        load_raw().wait()
        for target in range(owners):
            for slot in range(slots):
                f = (target * slots + slot) // row_split
                mine[target, :, slot : slot + 1, :] = raw[:, f : f + 1, :]
        pltpu.make_async_copy(mine.at[owner], places.at[owner], ids_recv).start()

        def send(k, carry):
            exchange_ids(lax.rem(owner + k, owners)).start()
            return carry

        lax.fori_loop(1, owners, send, 0)
        if kept:
            own = near_places.at[owner - base_owner]
            pltpu.make_async_copy(mine.at[mirror], own, near_recv).start()

            def send_near(k, carry):
                near_ids_copy(neighbour(k)).start()
                return carry

            lax.fori_loop(1, half, send_near, 0)

    def gather_ids():
        pltpu.make_async_copy(places, places, ids_recv).wait()
        for m in range(micro_count):
            for source in range(owners):
                ids[m, :, source * quarter : (source + 1) * quarter] = places[
                    source, m
                ]
        tacc[...] = jnp.zeros_like(tacc)
        if kept:
            pltpu.make_async_copy(near_places, near_places, near_recv).wait()
            for m in range(micro_count):
                for source in range(half):
                    near_ids[m, :, source * quarter : (source + 1) * quarter] = near_places[
                        source, m
                    ]
            nacc[...] = jnp.zeros_like(nacc)

    def collect(total, which, sources, first, rows, here, home):
        span = min(SPAN, sources * quarter)
        step = span // quarter

        def one(b, carry):
            at = first * quarter + b * span
            block_rows = rows[0][rows[1], pl.ds(first + b * step, step)]
            block_rows = block_rows.reshape(span, block_rows.shape[-1])
            for slot, target, lane in which:
                row_block = lax.rem(home * slots + slot, row_split)
                named = here[0][here[1], slot : slot + 1, pl.ds(pl.multiple_of(at, span), span)]
                positions = lax.broadcasted_iota(jnp.int32, (TROWS, span), 0)
                onehot = (positions == named - row_block * TROWS).astype(jnp.float32)
                total[target] += lax.dot_general(
                    onehot.astype(jnp.bfloat16),
                    block_rows[:, lane * width : (lane + 1) * width],
                    (((1,), (0,)), ((), ())), preferred_element_type=jnp.float32,
                )
            return carry

        lax.fori_loop(0, sources * quarter // span, one, 0)

    def tabulate(m):
        for j in range(per_micro):
            batch = arrived.at[m, :, pl.ds(j * PIECE, PIECE)]
            pltpu.make_async_copy(batch, batch, recv_sem.at[m * per_micro + j]).wait()
        with jax.named_scope("tabulate"):
            everyone = [(slot, slot, slot) for slot in range(direct)]
            collect(tacc, everyone, owners, 0, (arrived, m), (ids, m), owner)
            if kept:
                close = [(slot, slot, slot) for slot in range(direct, slots)]
                collect(tacc, close, half, base_owner, (arrived, m), (ids, m), owner)
                other = [(direct + i, i, i) for i in range(kept)]
                collect(nacc, other, half, 0, (near, m), (near_ids, m), mirror)

    def share_tables():
        for target in range(sections):
            @pl.when(section != target)
            def _():
                tsend[target] = tacc[:, target * share : (target + 1) * share, :].astype(jnp.bfloat16)
                share_copy(target).start()

            if kept:
                nsend[target] = nacc[:, target * share : (target + 1) * share, :].astype(jnp.bfloat16)
                near_share(target).start()

    with jax.named_scope("entry"):
        pl.semaphore_wait(barrier, owners - 1 + (sections - 1) * (2 if kept else 1))

    load_w().wait()

    @pl.when(section == last)
    def _():
        def first(m, carry):
            with jax.named_scope("head"):
                head(m)
            return carry

        def second(m, carry):
            with jax.named_scope("weigh"):
                weigh(m)
            return carry

        lax.fori_loop(0, micro_count, first, 0)
        lax.fori_loop(0, micro_count, second, 0)
        reduce_stage(0)
        send_ids()
        reduce_stage(1)

    @pl.when(section < last)
    def _():
        with jax.named_scope("turn"):
            wt[...] = w[...].T
        send_ids()
        for m in range(micro_count):
            load_pre(m).wait()

    lag = jnp.where((section == last) | (section == 0), 0, section * 2 + 1)
    most = last * 2 - 1

    def step(t, carry):
        @pl.when((section < last) & (t < chunks))
        def _():
            for i in range(subs):
                with jax.named_scope("chain"):
                    chain(t, i)

            @pl.when(lax.rem(t, per_micro) == per_micro - 1)
            def _():
                with jax.named_scope("weigh"):
                    weigh(t // per_micro)

            @pl.when(t == chunks - 1)
            def _():
                reduce_stage(0)

        p = t - lag

        @pl.when((p >= 0) & (p < chunks))
        def _():
            @pl.when(p == 0)
            def _():
                load_emb().wait()

            with jax.named_scope("pair"):
                pair(p)

        @pl.when((section < last) & (t == chunks))
        def _():
            reduce_stage(1, 0)

        for k in range(2, bits + 1):
            @pl.when((section == last) & (t == 5 * (k - 1)))
            def _():
                reduce_stage(k)

        @pl.when(p == per_micro)
        def _():
            with jax.named_scope("ids"):
                gather_ids()

        @pl.when((p >= 2 * per_micro) & (lax.rem(p, per_micro) == 0) & (p < chunks))
        def _():
            tabulate(p // per_micro - 2)

        return carry

    rounds = jnp.where(section == 0, chunks + 1, chunks + max(most, 5 * bits - chunks, 1))
    lax.fori_loop(0, rounds, step, 0)

    @pl.when(section < last)
    def _():
        reduce_stage(1, 1)

    @pl.when((section > 0) & (section < last))
    def _():
        reduce_stage(2, 0)

    tabulate(micro_count - 2)
    tabulate(micro_count - 1)
    share_tables()

    @pl.when(section == 0)
    def _():
        reduce_stage(2, 0)

    @pl.when(section < last)
    def _():
        reduce_stage(2, 1)
        for k in range(3, bits + 1):
            reduce_stage(k)

    wg_ref[...] = acc[block_of(0), :]

    here = pl.ds(pl.multiple_of(section * share, share), share)
    total = tacc[:, here, :]
    with jax.named_scope("shared"):
        for k in range(1, sections):
            source = lax.rem(section + k, sections)
            pltpu.make_async_copy(trecv.at[source], trecv.at[source], trecv_sem.at[source]).wait()
            total = total + trecv[source].astype(jnp.float32)
        table_ref[...] = total
        if kept:
            extra = jnp.zeros((kept, share, width), jnp.float32)
            for source in range(sections):
                pltpu.make_async_copy(nrecv.at[source], nrecv.at[source], nrecv_sem.at[source]).wait()
                extra = extra + nrecv[source].astype(jnp.float32)
            table_ref[direct:slots] = table_ref[direct:slots] + extra

    def drain_chain(u, carry):
        along(u).wait_send()
        return carry

    @pl.when(section > 0)
    def _():
        lax.fori_loop(0, chunks * subs, drain_chain, 0)

    def drain_hand(c, carry):
        sent = out_buf.at[c // per_micro, pl.ds(0, last), rows_of(lax.rem(c, per_micro))]
        pltpu.make_async_copy(sent, sent, hand_sem.at[c]).wait()
        return carry

    @pl.when(section == 0)
    def _():
        lax.fori_loop(0, chunks, drain_hand, 0)

    def drain_owner(k, carry):
        exchange_ids(lax.rem(owner + k, owners)).wait_send()
        reduce_copy(k, 0).wait_send()
        return carry

    lax.fori_loop(1, owners, drain_owner, 0)

    def drain_far(k, carry):
        target = lax.rem(neighbour(k) + half, owners)
        sent = outgoing.at[target, :, :, lanes(direct)]
        pltpu.make_async_copy(sent, sent, send_sem.at[target]).wait()
        return carry

    def drain_close(k, carry):
        target = neighbour(k)
        sent = outgoing.at[target]
        pltpu.make_async_copy(sent, sent, send_sem.at[target]).wait()
        if kept:
            sent = outgoing.at[target, :, :, pl.ds(direct * width, kept * width)]
            pltpu.make_async_copy(sent, sent, near_send.at[target]).wait()
            near_ids_copy(target).wait_send()
        return carry

    lax.fori_loop(0, half, drain_far, 0)
    lax.fori_loop(1, half, drain_close, 0)
    if kept:
        for target in range(sections):
            near_share(target).wait_send()
    for k in range(1, sections):
        share_copy(lax.rem(section + k, sections)).wait_send()


def scale_kernel(grad_scale, wg_ref, table_ref, wg_out, table_out):
    wg_out[...] = wg_ref[...] * grad_scale
    table_out[...] = table_ref[...] * grad_scale


def whole_step(layer_w, layer_pre, cotangent, layer_in, embeddings, row_ids, slots, row_split):
    sections = lax.axis_size("section")
    owners = lax.axis_size("owner")
    micro_count, batch_rows, hidden = cotangent.shape
    quarter, features, width = embeddings.shape[1:]
    chunks = micro_count * (quarter // PIECE)
    share = TROWS // sections
    kept = max(1, slots // PROXY)
    dims = (sections, owners, micro_count, quarter, features, width, slots, row_split)
    vmem = pl.BlockSpec(memory_space=pltpu.VMEM)
    anywhere = pl.BlockSpec(memory_space=pl.ANY)
    narrow, wide, whole = jnp.bfloat16, jnp.float32, jnp.int32
    split = (micro_count, sections, quarter, hidden)
    dma = pltpu.SemaphoreType.DMA
    return pl.pallas_call(
        functools.partial(step_kernel, dims),
        out_shape=(
            jax.ShapeDtypeStruct((hidden // owners, hidden), wide),
            jax.ShapeDtypeStruct((slots, share, width), wide),
        ),
        in_specs=[anywhere] * 6,
        out_specs=(vmem, vmem),
        scratch_shapes=[
            pltpu.VMEM((hidden, hidden), narrow),
            pltpu.VMEM((hidden, hidden), narrow),
            pltpu.VMEM(split, narrow),
            pltpu.VMEM(split, narrow),
            pltpu.VMEM((micro_count, batch_rows, hidden), narrow),
            pltpu.VMEM(embeddings.shape, narrow),
            pltpu.VMEM((micro_count, features, quarter), whole),
            pltpu.VMEM(split, narrow),
            pltpu.VMEM(split, narrow),
            pltpu.VMEM(split, narrow),
            pltpu.VMEM((chunks, PIECE, hidden), narrow),
            pltpu.VMEM((PIECE * features, 128), wide),
            pltpu.VMEM((PIECE * features, width), wide),
            pltpu.VMEM((owners, chunks, PIECE, slots * width), narrow),
            pltpu.VMEM((micro_count, owners, quarter, slots * width), narrow),
            pltpu.VMEM((micro_count, owners // 2, quarter, kept * width), narrow),
            pltpu.VMEM((owners, micro_count, slots, quarter), whole),
            pltpu.VMEM((owners, micro_count, slots, quarter), whole),
            pltpu.VMEM((owners // 2, micro_count, slots, quarter), whole),
            pltpu.VMEM((micro_count, slots, owners * quarter), whole),
            pltpu.VMEM((micro_count, slots, owners * quarter // 2), whole),
            pltpu.VMEM((hidden, hidden), wide),
            pltpu.VMEM((owners, hidden // owners, hidden), narrow),
            pltpu.VMEM((owners, hidden // owners, hidden), narrow),
            pltpu.VMEM((slots, TROWS, width), wide),
            pltpu.VMEM((kept, TROWS, width), wide),
            pltpu.VMEM((sections, slots, share, width), narrow),
            pltpu.VMEM((sections, slots, share, width), narrow),
            pltpu.VMEM((sections, kept, share, width), narrow),
            pltpu.VMEM((sections, kept, share, width), narrow),
            dma(()),
            dma((micro_count,)),
            dma((micro_count,)),
            dma(()),
            dma(()),
            dma(()),
            dma((chunks * sections // GROUP,)),
            dma((chunks * sections // GROUP,)),
            dma((chunks,)),
            dma((chunks,)),
            dma((owners,)),
            dma((chunks,)),
            dma((owners,)),
            dma(()),
            dma((owners,)),
            dma((owners,)),
            dma(()),
            dma((owners,)),
            dma((owners,)),
            dma((sections,)),
            dma((sections,)),
            dma((sections,)),
            dma((sections,)),
        ],
        compiler_params=pltpu.CompilerParams(
            collective_id=0, has_side_effects=True, vmem_limit_bytes=56 * 1024 * 1024
        ),
    )(
        layer_w, layer_pre.reshape(split), cotangent.reshape(split), layer_in, embeddings,
        jnp.swapaxes(row_ids, 1, 2),
    )


def per_device(weights, inputs, preact, cotangent, embeddings, row_ids):
    owners = lax.axis_size("owner")
    micro_count, batch_rows, hidden = cotangent.shape
    features = embeddings.shape[2]
    row_split = max(1, owners // features)
    slots = features * row_split // owners
    grad_scale = 1.0 / math.sqrt(micro_count * batch_rows * owners)
    weight_grad, table_grad = whole_step(
        weights[0], preact[0], cotangent, inputs[0], embeddings, row_ids, slots, row_split
    )
    vmem = pl.BlockSpec(memory_space=pltpu.VMEM)
    weight_grad, table_grad = pl.pallas_call(
        functools.partial(scale_kernel, grad_scale),
        out_shape=(
            jax.ShapeDtypeStruct(weight_grad.shape, jnp.float32),
            jax.ShapeDtypeStruct(table_grad.shape, jnp.float32),
        ),
        in_specs=[vmem, vmem],
        out_specs=(vmem, vmem),
    )(weight_grad, table_grad)
    return (weight_grad[None], table_grad)


def solution(mesh):
    return jax.shard_map(
        per_device,
        mesh=mesh,
        in_specs=(
            P("section", None, None),
            P("section", None, "owner", None),
            P("section", None, "owner", None),
            P(None, "owner", None),
            P(None, ("owner", "section"), None, None),
            P(None, ("owner", "section"), None),
        ),
        out_specs=(P("section", "owner", None), P("owner", "section", None)),
        check_vma=False,
    )
```

```python
import functools
import math

import jax
import jax.numpy as jnp
from jax import lax
from jax.experimental import pallas as pl
from jax.experimental.pallas import tpu as pltpu
from jax.sharding import PartitionSpec as P

TROWS = 512
PIECE = 16
SPAN = 512
GROUP = 2
PROXY = 4
SIDE = 4


def exclusive_or(a, b, bits):
    total = 0
    for k in range(bits):
        total = total + lax.rem(a // (1 << k) + b // (1 << k), 2) * (1 << k)
    return total


def step_kernel(
    dims, w_hbm, pre_hbm, cot_hbm, in_hbm, emb_hbm, ids_hbm, wg_ref, table_ref,
    w, wt, pre, cot, inp, emb, raw, slope, in_buf, out_buf, portion, square, pairs, outgoing,
    extra_out,
    arrived, near, mine, places, near_places, ids, near_ids, acc, wsend, wrecv, tacc, nacc,
    tsend, trecv, nsend, nrecv, side_send, side_recv, sum_send, sum_recv,
    w_sem, pre_sem, cot_sem, inp_sem, emb_sem, raw_sem, out_sem, in_sem, hand_sem, portion_sem,
    send_sem, recv_sem, close_sem, ids_send, ids_recv, near_send, near_ids_send, near_recv, wsend_sem, wrecv_sem,
    tsend_sem, trecv_sem, nsend_sem, nrecv_sem, side_out, side_in, sum_out, sum_in, ready,
):
    sections, owners, micro_count, quarter, features, width, slots, row_split = dims
    section = lax.axis_index("section")
    owner = lax.axis_index("owner")
    last = sections - 1
    lane_groups = 128 // features
    hidden = w.shape[0]
    per_micro = quarter // PIECE
    chunks = micro_count * per_micro
    subs = sections // GROUP
    bits = owners.bit_length() - 1
    block = hidden // owners
    share = TROWS // sections
    half = owners // 2
    kept = slots // PROXY
    direct = slots - kept
    main = hidden - hidden // SIDE // 128 * 128
    base_owner = owner // half * half
    mirror = lax.rem(owner + half, owners)

    barrier = pltpu.get_barrier_semaphore()
    for k in range(1, sections):
        pl.semaphore_signal(
            barrier, inc=1, device_id={"section": lax.rem(section + k, sections)},
            device_id_type=pl.DeviceIdType.MESH,
        )
    for k in range(1, owners):
        pl.semaphore_signal(
            barrier, inc=1, device_id={"owner": lax.rem(owner + k, owners)},
            device_id_type=pl.DeviceIdType.MESH,
        )

    if kept:
        for k in range(1, sections):
            pl.semaphore_signal(
                barrier, inc=1,
                device_id={"section": lax.rem(section + k, sections), "owner": mirror},
                device_id_type=pl.DeviceIdType.MESH,
            )

    def load_w():
        return pltpu.make_async_copy(w_hbm, w, w_sem)

    def load_pre(m):
        return pltpu.make_async_copy(pre_hbm.at[m], pre.at[m], pre_sem.at[m])

    def load_cot(m):
        return pltpu.make_async_copy(cot_hbm.at[m], cot.at[m], cot_sem.at[m])

    def load_inp():
        return pltpu.make_async_copy(in_hbm, inp, inp_sem)

    def load_emb():
        return pltpu.make_async_copy(emb_hbm, emb, emb_sem)

    def load_raw():
        return pltpu.make_async_copy(ids_hbm, raw, raw_sem)

    load_w().start()
    for m in range(micro_count):
        load_pre(m).start()

        @pl.when(section == last)
        def _():
            load_cot(m).start()

    load_raw().start()
    load_emb().start()
    load_inp().start()

    def rows_of(j):
        return pl.ds(pl.multiple_of(j * PIECE, PIECE), PIECE)

    def place(u):
        c = u // subs
        base = (subs - 1 - lax.rem(u, subs)) * GROUP
        return c // per_micro, pl.ds(base, GROUP), rows_of(lax.rem(c, per_micro))

    def along(u):
        at = place(u)
        return pltpu.make_async_remote_copy(
            src_ref=out_buf.at[at], dst_ref=in_buf.at[at],
            send_sem=out_sem.at[u], recv_sem=in_sem.at[u],
            device_id={"section": lax.rem(section + last, sections)},
            device_id_type=pl.DeviceIdType.MESH,
        )

    def hand(c, target):
        return pltpu.make_async_remote_copy(
            src_ref=out_buf.at[c // per_micro, target, rows_of(lax.rem(c, per_micro))],
            dst_ref=portion.at[c],
            send_sem=hand_sem.at[c], recv_sem=portion_sem.at[c],
            device_id={"section": target},
            device_id_type=pl.DeviceIdType.MESH,
        )

    def landing(c):
        return arrived.at[c // per_micro, owner, rows_of(lax.rem(c, per_micro))]

    def near_landing(c):
        return near.at[c // per_micro, owner - base_owner, rows_of(lax.rem(c, per_micro))]

    def exchange(c, target):
        return pltpu.make_async_remote_copy(
            src_ref=outgoing.at[target, c], dst_ref=landing(c),
            send_sem=send_sem.at[target], recv_sem=recv_sem.at[c],
            device_id={"owner": target},
            device_id_type=pl.DeviceIdType.MESH,
        )

    def exchange_near(c, target):
        return pltpu.make_async_remote_copy(
            src_ref=extra_out.at[target, c], dst_ref=near_landing(c),
            send_sem=near_send.at[target], recv_sem=close_sem.at[c],
            device_id={"owner": target},
            device_id_type=pl.DeviceIdType.MESH,
        )

    def exchange_ids(target):
        return pltpu.make_async_remote_copy(
            src_ref=mine.at[target], dst_ref=places.at[owner],
            send_sem=ids_send.at[target], recv_sem=ids_recv,
            device_id={"owner": target},
            device_id_type=pl.DeviceIdType.MESH,
        )

    def near_ids_copy(target):
        return pltpu.make_async_remote_copy(
            src_ref=mine.at[lax.rem(target + half, owners)],
            dst_ref=near_places.at[owner - base_owner],
            send_sem=near_ids_send.at[target], recv_sem=near_recv,
            device_id={"owner": target},
            device_id_type=pl.DeviceIdType.MESH,
        )

    def reduce_copy(d, k, count):
        across = pl.ds(0, count)
        return pltpu.make_async_remote_copy(
            src_ref=wsend.at[d, :, across], dst_ref=wrecv.at[d, :, across],
            send_sem=wsend_sem.at[d], recv_sem=wrecv_sem.at[d],
            device_id={"owner": exclusive_or(owner, 1 << k, bits)},
            device_id_type=pl.DeviceIdType.MESH,
        )

    def side_copy(h):
        return pltpu.make_async_remote_copy(
            src_ref=side_send.at[h], dst_ref=side_recv.at[section, h],
            send_sem=side_out.at[h], recv_sem=side_in.at[section, h],
            device_id={"section": last, "owner": exclusive_or(owner, 2 * h, bits)},
            device_id_type=pl.DeviceIdType.MESH,
        )

    def sum_copy(target):
        return pltpu.make_async_remote_copy(
            src_ref=sum_send.at[target], dst_ref=sum_recv,
            send_sem=sum_out.at[target], recv_sem=sum_in,
            device_id={"section": target},
            device_id_type=pl.DeviceIdType.MESH,
        )

    def share_copy(target):
        return pltpu.make_async_remote_copy(
            src_ref=tsend.at[target], dst_ref=trecv.at[section],
            send_sem=tsend_sem.at[target], recv_sem=trecv_sem.at[section],
            device_id={"section": target},
            device_id_type=pl.DeviceIdType.MESH,
        )

    def near_share(target):
        return pltpu.make_async_remote_copy(
            src_ref=nsend.at[target], dst_ref=nrecv.at[section],
            send_sem=nsend_sem.at[target], recv_sem=nrecv_sem.at[section],
            device_id={"section": target, "owner": mirror},
            device_id_type=pl.DeviceIdType.MESH,
        )

    def neighbour(k):
        return base_owner + lax.rem(owner - base_owner + k, half)

    def head(m):
        load_pre(m).wait()
        load_cot(m).wait()
        positive = pre[m].astype(jnp.float32) > 0
        slope[m] = jnp.where(positive, cot[m].astype(jnp.float32), 0.0).astype(jnp.bfloat16)
        out_buf[m] = lax.dot_general(
            slope[m].reshape(sections * quarter, hidden), w[...], (((1,), (1,)), ((), ())),
            preferred_element_type=jnp.float32,
        ).astype(jnp.bfloat16).reshape(sections, quarter, hidden)

        def send(i, carry):
            along(m * per_micro * subs + i).start()
            return carry

        lax.fori_loop(0, per_micro * subs, send, 0)

    def chain(c, i):
        u = c * subs + i
        m, j = c // per_micro, lax.rem(c, per_micro)
        base = (subs - 1 - i) * GROUP
        at = (m, pl.ds(base, GROUP), rows_of(j))
        positive = pre[at].astype(jnp.float32) > 0
        with jax.named_scope("arrive"):
            along(u).wait_recv()
        grad = in_buf[at].astype(jnp.float32)
        slope[at] = jnp.where(positive, grad, 0.0).astype(jnp.bfloat16)
        out_buf[at] = lax.dot_general(
            slope[at].reshape(GROUP * PIECE, hidden), wt[...], (((1,), (0,)), ((), ())),
            preferred_element_type=jnp.float32,
        ).astype(jnp.bfloat16).reshape(GROUP, PIECE, hidden)

        @pl.when(section > 0)
        def _():
            along(u).start()

        @pl.when(section == 0)
        def _():
            for target in range(base, base + GROUP):
                if target == 0:
                    portion[c] = out_buf[m, 0, rows_of(j)]
                else:
                    hand(c, target).start()

    def pair(c):
        m, j = c // per_micro, lax.rem(c, per_micro)

        @pl.when(section > 0)
        def _():
            with jax.named_scope("handed"):
                hand(c, 0).wait_recv()

        for f in range(features):
            group, part = f // lane_groups, f % lane_groups
            piece = portion[c, :, group * 128 : (group + 1) * 128].astype(jnp.float32)
            if part:
                piece = pltpu.roll(piece, 128 - part * features, 1)
            square[pl.ds(f, PIECE, stride=features), :] = piece
        whole = square[...].reshape(PIECE, features, 128)[:, :, :features]
        both = (whole + jnp.swapaxes(whole, 1, 2)).astype(jnp.bfloat16)
        pairs[...] = lax.dot_general(
            both, emb[m, rows_of(j)], (((2,), (1,)), ((0,), (0,))),
            preferred_element_type=jnp.float32,
        ).reshape(PIECE * features, width)
        def rows_for(f):
            return pairs[pl.ds(f, PIECE, stride=features), :].astype(jnp.bfloat16)

        for target in range(owners):
            for slot in range(direct):
                f = (target * slots + slot) // row_split
                outgoing[target, c, :, slot * width : (slot + 1) * width] = rows_for(f)
        opposite = [(target + half) % owners for target in range(owners)]
        for target in range(owners):
            for slot in range(kept):
                f = (target * slots + direct + slot) // row_split
                made = rows_for(f)
                extra_out[target, c, :, slot * width : (slot + 1) * width] = made
                lane = (kept + slot) * width
                extra_out[opposite[target], c, :, lane : lane + width] = made

        def send_far(k, carry):
            exchange(c, lax.rem(neighbour(k) + half, owners)).start()
            return carry

        def send_close(k, carry):
            exchange(c, neighbour(k)).start()
            if kept:
                exchange_near(c, neighbour(k)).start()
            return carry

        lax.fori_loop(0, half, send_far, 0)
        lax.fori_loop(1, half, send_close, 0)
        pltpu.make_async_copy(outgoing.at[owner, c], landing(c), recv_sem.at[c]).start()
        if kept:
            pltpu.make_async_copy(extra_out.at[owner, c], near_landing(c), close_sem.at[c]).start()

    def weigh(m):
        def product():
            return lax.dot_general(
                inp[m], slope[m].reshape(sections * quarter, hidden), (((0,), (0,)), ((), ())),
                preferred_element_type=jnp.float32,
            )

        @pl.when(m == 0)
        def _():
            load_inp().wait()
            acc[...] = product()

        @pl.when(m > 0)
        def _():
            acc[...] += product()

    def block_of(d):
        at = exclusive_or(owner, d, bits) * block
        return pl.ds(pl.multiple_of(at, block), block)

    def send_block(d, k, count):
        wsend[d, :, :count] = acc[block_of(d), :count].astype(jnp.bfloat16)
        reduce_copy(d, k, count).start()

    def reduce_stage(k, part=None, full=False):
        held = owners >> k
        top = held // 2 if part == 1 else held
        count = held if part is None else held // 2

        def across(stage):
            return hidden if full or stage == 0 else main

        def one(i, carry):
            h = top - 1 - i
            if k > 0:
                d = (1 << (k - 1)) + h * (1 << k)
                come = across(k - 1)
                reduce_copy(d, k - 1, come).wait_recv()
                at = block_of(h * (1 << k))
                acc[at, :come] = acc[at, :come] + wrecv[d, :, :come].astype(jnp.float32)
            if k < bits:
                ahead = h >= held // 2 if k == 1 and not full else True
                @pl.when((lax.rem(h, 2) == 1) & ahead)
                def _():
                    send_block(h * (1 << k), k, across(k))
            if k == 1 and not full:
                @pl.when(h > 0)
                def _():
                    side_send[h] = acc[block_of(h * 2), main:].astype(jnp.bfloat16)
                    side_copy(h).start()

            return carry

        with jax.named_scope(f"reduce{k}"):
            lax.fori_loop(0, count, one, 0)

    def send_rest():
        with jax.named_scope("rest"):
            for h in range(1, half // 2, 2):
                send_block(2 * h, 1, main)

    def side_sum(source):
        with jax.named_scope("side"):
            total = jnp.zeros((block, hidden - main), jnp.float32)
            for h in range(1, half):
                landed = side_recv.at[source, h]
                pltpu.make_async_copy(landed, landed, side_in.at[source, h]).wait()
                total = total + side_recv[source, h].astype(jnp.float32)
            sum_send[source] = total.astype(jnp.bfloat16)
            sum_copy(source).start()

    def send_ids():
        load_raw().wait()
        for target in range(owners):
            for slot in range(slots):
                f = (target * slots + slot) // row_split
                mine[target, :, slot : slot + 1, :] = raw[:, f : f + 1, :]
        pltpu.make_async_copy(mine.at[owner], places.at[owner], ids_recv).start()

        def send(k, carry):
            exchange_ids(lax.rem(owner + k, owners)).start()
            return carry

        lax.fori_loop(1, owners, send, 0)
        if kept:
            own = near_places.at[owner - base_owner]
            pltpu.make_async_copy(mine.at[mirror], own, near_recv).start()

            def send_near(k, carry):
                near_ids_copy(neighbour(k)).start()
                return carry

            lax.fori_loop(1, half, send_near, 0)

    def gather_ids():
        pltpu.make_async_copy(places, places, ids_recv).wait()
        for m in range(micro_count):
            for source in range(owners):
                ids[m, :, source * quarter : (source + 1) * quarter] = places[
                    source, m
                ]
        tacc[...] = jnp.zeros_like(tacc)
        if kept:
            pltpu.make_async_copy(near_places, near_places, near_recv).wait()
            for m in range(micro_count):
                for source in range(half):
                    near_ids[m, :, source * quarter : (source + 1) * quarter] = near_places[
                        source, m
                    ]
            nacc[...] = jnp.zeros_like(nacc)

    def collect(total, which, sources, first, rows, here, home, base=None):
        span = min(SPAN, sources * quarter)
        step = span // quarter

        def one(b, carry):
            at = first * quarter + b * span
            start = first if base is None else base
            block_rows = rows[0][rows[1], pl.ds(start + b * step, step)]
            block_rows = block_rows.reshape(span, block_rows.shape[-1])
            for slot, target, lane in which:
                row_block = lax.rem(home * slots + slot, row_split)
                named = here[0][here[1], slot : slot + 1, pl.ds(pl.multiple_of(at, span), span)]
                positions = lax.broadcasted_iota(jnp.int32, (TROWS, span), 0)
                onehot = (positions == named - row_block * TROWS).astype(jnp.float32)
                total[target] += lax.dot_general(
                    onehot.astype(jnp.bfloat16),
                    block_rows[:, lane * width : (lane + 1) * width],
                    (((1,), (0,)), ((), ())), preferred_element_type=jnp.float32,
                )
            return carry

        lax.fori_loop(0, sources * quarter // span, one, 0)

    def tabulate(m):
        for j in range(per_micro):
            batch = arrived.at[m, :, pl.ds(j * PIECE, PIECE)]
            pltpu.make_async_copy(batch, batch, recv_sem.at[m * per_micro + j]).wait()
            if kept:
                batch = near.at[m, :, pl.ds(j * PIECE, PIECE)]
                pltpu.make_async_copy(batch, batch, close_sem.at[m * per_micro + j]).wait()
        with jax.named_scope("tabulate"):
            everyone = [(slot, slot, slot) for slot in range(direct)]
            collect(tacc, everyone, owners, 0, (arrived, m), (ids, m), owner)
            if kept:
                close = [(direct + i, direct + i, i) for i in range(kept)]
                collect(tacc, close, half, base_owner, (near, m), (ids, m), owner, 0)
                other = [(direct + i, i, kept + i) for i in range(kept)]
                collect(nacc, other, half, 0, (near, m), (near_ids, m), mirror)

    def share_tables():
        for target in range(sections):
            @pl.when(section != target)
            def _():
                tsend[target] = tacc[:, target * share : (target + 1) * share, :].astype(jnp.bfloat16)
                share_copy(target).start()

            if kept:
                nsend[target] = nacc[:, target * share : (target + 1) * share, :].astype(jnp.bfloat16)
                near_share(target).start()

    with jax.named_scope("entry"):
        pl.semaphore_wait(barrier, owners - 1 + (sections - 1) * (2 if kept else 1))

    @pl.when(section == last)
    def _():
        for target in range(last):
            pl.semaphore_signal(
                ready, inc=1, device_id={"section": target},
                device_id_type=pl.DeviceIdType.MESH,
            )

    load_w().wait()

    @pl.when(section == last)
    def _():
        def first(m, carry):
            with jax.named_scope("head"):
                head(m)
            return carry

        def second(m, carry):
            with jax.named_scope("weigh"):
                weigh(m)
            return carry

        lax.fori_loop(0, micro_count, first, 0)
        lax.fori_loop(0, micro_count, second, 0)
        reduce_stage(0, None, True)
        send_ids()
        reduce_stage(1, None, True)

    @pl.when(section < last)
    def _():
        with jax.named_scope("turn"):
            wt[...] = w[...].T
        send_ids()
        for m in range(micro_count):
            load_pre(m).wait()
        pl.semaphore_wait(ready, 1)

    lag = jnp.where((section == last) | (section == 0), 0, section * 2 + 1)
    most = last * 2 - 1

    def step(t, carry):
        @pl.when((section < last) & (t < chunks))
        def _():
            for i in range(subs):
                with jax.named_scope("chain"):
                    chain(t, i)

            @pl.when(lax.rem(t, per_micro) == per_micro - 1)
            def _():
                with jax.named_scope("weigh"):
                    weigh(t // per_micro)

            @pl.when(t == chunks - 1)
            def _():
                reduce_stage(0)

        p = t - lag

        @pl.when((p >= 0) & (p < chunks))
        def _():
            @pl.when(p == 0)
            def _():
                load_emb().wait()

            with jax.named_scope("pair"):
                pair(p)

        @pl.when((section < last) & (t == chunks))
        def _():
            reduce_stage(1)

        for k in range(2, bits + 1):
            @pl.when((section == last) & (t == 5 * (k - 1)))
            def _():
                reduce_stage(k, None, True)

        @pl.when(p == per_micro)
        def _():
            with jax.named_scope("ids"):
                gather_ids()

        @pl.when((p >= 2 * per_micro) & (lax.rem(p, per_micro) == 0) & (p < chunks))
        def _():
            tabulate(p // per_micro - 2)

        return carry

    rounds = jnp.where(section == 0, chunks + 1, chunks + max(most, 5 * bits - chunks, 1))
    lax.fori_loop(0, rounds, step, 0)

    @pl.when((section > 0) & (section < last))
    def _():
        reduce_stage(2, 0)

    tabulate(micro_count - 2)
    tabulate(micro_count - 1)
    share_tables()

    @pl.when(section == last)
    def _():
        for source in range(last - 1, -1, -1):
            side_sum(source)

    @pl.when(section < last)
    def _():
        send_rest()

    @pl.when(section == 0)
    def _():
        reduce_stage(2, 0)

    def drain_chain(u, carry):
        along(u).wait_send()
        return carry

    @pl.when(section > 0)
    def _():
        lax.fori_loop(0, chunks * subs, drain_chain, 0)

    def drain_hand(c, carry):
        sent = out_buf.at[c // per_micro, pl.ds(0, last), rows_of(lax.rem(c, per_micro))]
        pltpu.make_async_copy(sent, sent, hand_sem.at[c]).wait()
        return carry

    @pl.when(section == 0)
    def _():
        lax.fori_loop(0, chunks, drain_hand, 0)

    def drain_far(k, carry):
        target = lax.rem(neighbour(k) + half, owners)
        sent = outgoing.at[target]
        pltpu.make_async_copy(sent, sent, send_sem.at[target]).wait()
        return carry

    def drain_close(k, carry):
        target = neighbour(k)
        sent = outgoing.at[target]
        pltpu.make_async_copy(sent, sent, send_sem.at[target]).wait()
        if kept:
            sent = extra_out.at[target]
            pltpu.make_async_copy(sent, sent, near_send.at[target]).wait()
            near_ids_copy(target).wait_send()
        return carry

    lax.fori_loop(0, half, drain_far, 0)
    lax.fori_loop(1, half, drain_close, 0)

    @pl.when(section < last)
    def _():
        reduce_stage(2, 1)
        for k in range(3, bits + 1):
            reduce_stage(k)
        with jax.named_scope("sum"):
            pltpu.make_async_copy(sum_recv, sum_recv, sum_in).wait()
            acc[block_of(0), main:] = acc[block_of(0), main:] + sum_recv[...].astype(jnp.float32)

    wg_ref[...] = acc[block_of(0), :]

    here = pl.ds(pl.multiple_of(section * share, share), share)
    total = tacc[:, here, :]
    with jax.named_scope("shared"):
        for k in range(1, sections):
            source = lax.rem(section + k, sections)
            pltpu.make_async_copy(trecv.at[source], trecv.at[source], trecv_sem.at[source]).wait()
            total = total + trecv[source].astype(jnp.float32)
        table_ref[...] = total
        if kept:
            extra = jnp.zeros((kept, share, width), jnp.float32)
            for source in range(sections):
                pltpu.make_async_copy(nrecv.at[source], nrecv.at[source], nrecv_sem.at[source]).wait()
                extra = extra + nrecv[source].astype(jnp.float32)
            table_ref[direct:slots] = table_ref[direct:slots] + extra

    def drain_owner(k, carry):
        exchange_ids(lax.rem(owner + k, owners)).wait_send()
        return carry

    lax.fori_loop(1, owners, drain_owner, 0)


    def drain_blocks(full):
        for k in range(bits):
            for h in range(owners >> (k + 1)):
                count = hidden if full or k == 0 else main
                reduce_copy((1 << k) + h * (2 << k), k, count).wait_send()

    @pl.when(section == last)
    def _():
        drain_blocks(True)
        for target in range(last):
            sum_copy(target).wait_send()

    @pl.when(section < last)
    def _():
        drain_blocks(False)
        for h in range(1, half):
            side_copy(h).wait_send()

    if kept:
        for target in range(sections):
            near_share(target).wait_send()
    for k in range(1, sections):
        share_copy(lax.rem(section + k, sections)).wait_send()


def scale_kernel(grad_scale, wg_ref, table_ref, wg_out, table_out):
    wg_out[...] = wg_ref[...] * grad_scale
    table_out[...] = table_ref[...] * grad_scale


def whole_step(layer_w, layer_pre, cotangent, layer_in, embeddings, row_ids, slots, row_split):
    sections = lax.axis_size("section")
    owners = lax.axis_size("owner")
    micro_count, batch_rows, hidden = cotangent.shape
    quarter, features, width = embeddings.shape[1:]
    chunks = micro_count * (quarter // PIECE)
    share = TROWS // sections
    direct = slots - slots // PROXY
    block, aside = hidden // owners, hidden // SIDE // 128 * 128
    kept = max(1, slots // PROXY)
    dims = (sections, owners, micro_count, quarter, features, width, slots, row_split)
    vmem = pl.BlockSpec(memory_space=pltpu.VMEM)
    anywhere = pl.BlockSpec(memory_space=pltpu.HBM)
    narrow, wide, whole = jnp.bfloat16, jnp.float32, jnp.int32
    split = (micro_count, sections, quarter, hidden)
    dma = pltpu.SemaphoreType.DMA
    return pl.pallas_call(
        functools.partial(step_kernel, dims),
        out_shape=(
            jax.ShapeDtypeStruct((hidden // owners, hidden), wide),
            jax.ShapeDtypeStruct((slots, share, width), wide),
        ),
        in_specs=[anywhere] * 6,
        out_specs=(vmem, vmem),
        scratch_shapes=[
            pltpu.VMEM((hidden, hidden), narrow),
            pltpu.VMEM((hidden, hidden), narrow),
            pltpu.VMEM(split, narrow),
            pltpu.VMEM(split, narrow),
            pltpu.VMEM((micro_count, batch_rows, hidden), narrow),
            pltpu.VMEM(embeddings.shape, narrow),
            pltpu.VMEM((micro_count, features, quarter), whole),
            pltpu.VMEM(split, narrow),
            pltpu.VMEM(split, narrow),
            pltpu.VMEM(split, narrow),
            pltpu.VMEM((chunks, PIECE, hidden), narrow),
            pltpu.VMEM((PIECE * features, 128), wide),
            pltpu.VMEM((PIECE * features, width), wide),
            pltpu.VMEM((owners, chunks, PIECE, direct * width), narrow),
            pltpu.VMEM((owners, chunks, PIECE, 2 * kept * width), narrow),
            pltpu.VMEM((micro_count, owners, quarter, direct * width), narrow),
            pltpu.VMEM((micro_count, owners // 2, quarter, 2 * kept * width), narrow),
            pltpu.VMEM((owners, micro_count, slots, quarter), whole),
            pltpu.VMEM((owners, micro_count, slots, quarter), whole),
            pltpu.VMEM((owners // 2, micro_count, slots, quarter), whole),
            pltpu.VMEM((micro_count, slots, owners * quarter), whole),
            pltpu.VMEM((micro_count, slots, owners * quarter // 2), whole),
            pltpu.VMEM((hidden, hidden), wide),
            pltpu.VMEM((owners, hidden // owners, hidden), narrow),
            pltpu.VMEM((owners, hidden // owners, hidden), narrow),
            pltpu.VMEM((slots, TROWS, width), wide),
            pltpu.VMEM((kept, TROWS, width), wide),
            pltpu.VMEM((sections, slots, share, width), narrow),
            pltpu.VMEM((sections, slots, share, width), narrow),
            pltpu.VMEM((sections, kept, share, width), narrow),
            pltpu.VMEM((sections, kept, share, width), narrow),
            pltpu.VMEM((owners // 2, block, aside), narrow),
            pltpu.VMEM((sections - 1, owners // 2, block, aside), narrow),
            pltpu.VMEM((sections - 1, block, aside), narrow),
            pltpu.VMEM((block, aside), narrow),
            dma(()),
            dma((micro_count,)),
            dma((micro_count,)),
            dma(()),
            dma(()),
            dma(()),
            dma((chunks * sections // GROUP,)),
            dma((chunks * sections // GROUP,)),
            dma((chunks,)),
            dma((chunks,)),
            dma((owners,)),
            dma((chunks,)),
            dma((chunks,)),
            dma((owners,)),
            dma(()),
            dma((owners,)),
            dma((owners,)),
            dma(()),
            dma((owners,)),
            dma((owners,)),
            dma((sections,)),
            dma((sections,)),
            dma((sections,)),
            dma((sections,)),
            dma((owners // 2,)),
            dma((sections - 1, owners // 2)),
            dma((sections - 1,)),
            dma(()),
            pltpu.SemaphoreType.REGULAR,
        ],
        compiler_params=pltpu.CompilerParams(
            collective_id=0, has_side_effects=True, vmem_limit_bytes=54272 * 1024
        ),
    )(
        layer_w, layer_pre.reshape(split), cotangent.reshape(split), layer_in, embeddings,
        jnp.swapaxes(row_ids, 1, 2),
    )


def per_device(weights, inputs, preact, cotangent, embeddings, row_ids):
    owners = lax.axis_size("owner")
    micro_count, batch_rows, hidden = cotangent.shape
    features = embeddings.shape[2]
    row_split = max(1, owners // features)
    slots = features * row_split // owners
    grad_scale = 1.0 / math.sqrt(micro_count * batch_rows * owners)
    weight_grad, table_grad = whole_step(
        weights[0], preact[0], cotangent, inputs[0], embeddings, row_ids, slots, row_split
    )
    vmem = pl.BlockSpec(memory_space=pltpu.VMEM)
    weight_grad, table_grad = pl.pallas_call(
        functools.partial(scale_kernel, grad_scale),
        out_shape=(
            jax.ShapeDtypeStruct(weight_grad.shape, jnp.float32),
            jax.ShapeDtypeStruct(table_grad.shape, jnp.float32),
        ),
        in_specs=[vmem, vmem],
        out_specs=(vmem, vmem),
        compiler_params=pltpu.CompilerParams(vmem_limit_bytes=8 * 1024 * 1024),
    )(weight_grad, table_grad)
    return (weight_grad[None], table_grad)


def solution(mesh):
    return jax.shard_map(
        per_device,
        mesh=mesh,
        in_specs=(
            P("section", None, None),
            P("section", None, "owner", None),
            P("section", None, "owner", None),
            P(None, "owner", None),
            P(None, ("owner", "section"), None, None),
            P(None, ("owner", "section"), None),
        ),
        out_specs=(P("section", "owner", None), P("owner", "section", None)),
        check_vma=False,
    )
```

```python
import functools
import math

import jax
import jax.numpy as jnp
from jax import lax
from jax.experimental import pallas as pl
from jax.experimental.pallas import tpu as pltpu
from jax.sharding import PartitionSpec as P

TROWS = 512
PIECE = 16
SPAN = 512
GROUP = 2
PROXY = 4
SIDE = 4


def exclusive_or(a, b, bits):
    total = 0
    for k in range(bits):
        total = total + lax.rem(a // (1 << k) + b // (1 << k), 2) * (1 << k)
    return total


def step_kernel(
    dims, w_hbm, pre_hbm, cot_hbm, in_hbm, emb_hbm, ids_hbm, wg_ref, table_ref,
    w, wt, pre, cot, inp, emb, raw, slope, in_buf, out_buf, portion, square, pairs, outgoing,
    extra_out,
    arrived, near, mine, places, near_places, ids, near_ids, acc, wsend, wrecv, tacc, nacc,
    tsend, trecv, nsend, nrecv, side_send, side_recv, sum_send, sum_recv,
    w_sem, pre_sem, cot_sem, inp_sem, emb_sem, raw_sem, out_sem, in_sem, hand_sem, portion_sem,
    send_sem, recv_sem, close_sem, ids_send, ids_recv, near_send, near_ids_send, near_recv, wsend_sem, wrecv_sem,
    tsend_sem, trecv_sem, nsend_sem, nrecv_sem, side_out, side_in, sum_out, sum_in, ready,
):
    sections, owners, micro_count, quarter, features, width, slots, row_split = dims
    section = lax.axis_index("section")
    owner = lax.axis_index("owner")
    last = sections - 1
    lane_groups = 128 // features
    hidden = w.shape[0]
    per_micro = quarter // PIECE
    chunks = micro_count * per_micro
    subs = sections // GROUP
    bits = owners.bit_length() - 1
    block = hidden // owners
    share = TROWS // sections
    half = owners // 2
    kept = slots // PROXY
    direct = slots - kept
    main = hidden - hidden // SIDE // 128 * 128
    base_owner = owner // half * half
    mirror = lax.rem(owner + half, owners)

    barrier = pltpu.get_barrier_semaphore()
    for k in range(1, sections):
        pl.semaphore_signal(
            barrier, inc=1, device_id={"section": lax.rem(section + k, sections)},
            device_id_type=pl.DeviceIdType.MESH,
        )
    for k in range(1, owners):
        pl.semaphore_signal(
            barrier, inc=1, device_id={"owner": lax.rem(owner + k, owners)},
            device_id_type=pl.DeviceIdType.MESH,
        )

    if kept:
        for k in range(1, sections):
            pl.semaphore_signal(
                barrier, inc=1,
                device_id={"section": lax.rem(section + k, sections), "owner": mirror},
                device_id_type=pl.DeviceIdType.MESH,
            )

    def load_w():
        return pltpu.make_async_copy(w_hbm, w, w_sem)

    def load_pre(m):
        return pltpu.make_async_copy(pre_hbm.at[m], pre.at[m], pre_sem.at[m])

    def load_cot(m):
        return pltpu.make_async_copy(cot_hbm.at[m], cot.at[m], cot_sem.at[m])

    def load_inp():
        return pltpu.make_async_copy(in_hbm, inp, inp_sem)

    def load_emb():
        return pltpu.make_async_copy(emb_hbm, emb, emb_sem)

    def load_raw():
        return pltpu.make_async_copy(ids_hbm, raw, raw_sem)

    load_w().start()
    for m in range(micro_count):
        load_pre(m).start()

        @pl.when(section == last)
        def _():
            load_cot(m).start()

    load_raw().start()
    load_emb().start()
    load_inp().start()

    def rows_of(j):
        return pl.ds(pl.multiple_of(j * PIECE, PIECE), PIECE)

    def place(u):
        c = u // subs
        base = (subs - 1 - lax.rem(u, subs)) * GROUP
        return c // per_micro, pl.ds(base, GROUP), rows_of(lax.rem(c, per_micro))

    def along(u):
        at = place(u)
        return pltpu.make_async_remote_copy(
            src_ref=out_buf.at[at], dst_ref=in_buf.at[at],
            send_sem=out_sem.at[u], recv_sem=in_sem.at[u],
            device_id={"section": lax.rem(section + last, sections)},
            device_id_type=pl.DeviceIdType.MESH,
        )

    def hand(c, target):
        return pltpu.make_async_remote_copy(
            src_ref=out_buf.at[c // per_micro, target, rows_of(lax.rem(c, per_micro))],
            dst_ref=portion.at[c],
            send_sem=hand_sem.at[c], recv_sem=portion_sem.at[c],
            device_id={"section": target},
            device_id_type=pl.DeviceIdType.MESH,
        )

    def landing(c):
        return arrived.at[c // per_micro, owner, rows_of(lax.rem(c, per_micro))]

    def near_landing(c):
        return near.at[c // per_micro, owner - base_owner, rows_of(lax.rem(c, per_micro))]

    def exchange(c, target):
        return pltpu.make_async_remote_copy(
            src_ref=outgoing.at[target, c], dst_ref=landing(c),
            send_sem=send_sem.at[target], recv_sem=recv_sem.at[c],
            device_id={"owner": target},
            device_id_type=pl.DeviceIdType.MESH,
        )

    def exchange_near(c, target):
        return pltpu.make_async_remote_copy(
            src_ref=extra_out.at[target, c], dst_ref=near_landing(c),
            send_sem=near_send.at[target], recv_sem=close_sem.at[c],
            device_id={"owner": target},
            device_id_type=pl.DeviceIdType.MESH,
        )

    def exchange_ids(target):
        return pltpu.make_async_remote_copy(
            src_ref=mine.at[target], dst_ref=places.at[owner],
            send_sem=ids_send.at[target], recv_sem=ids_recv,
            device_id={"owner": target},
            device_id_type=pl.DeviceIdType.MESH,
        )

    def near_ids_copy(target):
        return pltpu.make_async_remote_copy(
            src_ref=mine.at[lax.rem(target + half, owners)],
            dst_ref=near_places.at[owner - base_owner],
            send_sem=near_ids_send.at[target], recv_sem=near_recv,
            device_id={"owner": target},
            device_id_type=pl.DeviceIdType.MESH,
        )

    def reduce_copy(d, k, count):
        across = pl.ds(0, count)
        return pltpu.make_async_remote_copy(
            src_ref=wsend.at[d, :, across], dst_ref=wrecv.at[d, :, across],
            send_sem=wsend_sem.at[d], recv_sem=wrecv_sem.at[d],
            device_id={"owner": exclusive_or(owner, 1 << k, bits)},
            device_id_type=pl.DeviceIdType.MESH,
        )

    def side_copy(h):
        return pltpu.make_async_remote_copy(
            src_ref=side_send.at[h], dst_ref=side_recv.at[section, h],
            send_sem=side_out.at[h], recv_sem=side_in.at[section, h],
            device_id={"section": last, "owner": exclusive_or(owner, 2 * h, bits)},
            device_id_type=pl.DeviceIdType.MESH,
        )

    def sum_copy(target):
        return pltpu.make_async_remote_copy(
            src_ref=sum_send.at[target], dst_ref=sum_recv,
            send_sem=sum_out.at[target], recv_sem=sum_in,
            device_id={"section": target},
            device_id_type=pl.DeviceIdType.MESH,
        )

    def share_copy(target):
        return pltpu.make_async_remote_copy(
            src_ref=tsend.at[target], dst_ref=trecv.at[section],
            send_sem=tsend_sem.at[target], recv_sem=trecv_sem.at[section],
            device_id={"section": target},
            device_id_type=pl.DeviceIdType.MESH,
        )

    def near_share(target):
        return pltpu.make_async_remote_copy(
            src_ref=nsend.at[target], dst_ref=nrecv.at[section],
            send_sem=nsend_sem.at[target], recv_sem=nrecv_sem.at[section],
            device_id={"section": target, "owner": mirror},
            device_id_type=pl.DeviceIdType.MESH,
        )

    def neighbour(k):
        return base_owner + lax.rem(owner - base_owner + k, half)

    def head(m):
        load_pre(m).wait()
        load_cot(m).wait()
        positive = pre[m].astype(jnp.float32) > 0
        slope[m] = jnp.where(positive, cot[m].astype(jnp.float32), 0.0).astype(jnp.bfloat16)
        out_buf[m] = lax.dot_general(
            slope[m].reshape(sections * quarter, hidden), w[...], (((1,), (1,)), ((), ())),
            preferred_element_type=jnp.float32,
        ).astype(jnp.bfloat16).reshape(sections, quarter, hidden)

        def send(i, carry):
            along(m * per_micro * subs + i).start()
            return carry

        lax.fori_loop(0, per_micro * subs, send, 0)

    def chain(c, i):
        u = c * subs + i
        m, j = c // per_micro, lax.rem(c, per_micro)
        base = (subs - 1 - i) * GROUP
        at = (m, pl.ds(base, GROUP), rows_of(j))
        positive = pre[at].astype(jnp.float32) > 0
        with jax.named_scope("arrive"):
            along(u).wait_recv()
        grad = in_buf[at].astype(jnp.float32)
        slope[at] = jnp.where(positive, grad, 0.0).astype(jnp.bfloat16)
        out_buf[at] = lax.dot_general(
            slope[at].reshape(GROUP * PIECE, hidden), wt[...], (((1,), (0,)), ((), ())),
            preferred_element_type=jnp.float32,
        ).astype(jnp.bfloat16).reshape(GROUP, PIECE, hidden)

        @pl.when(section > 0)
        def _():
            along(u).start()

        @pl.when(section == 0)
        def _():
            for target in range(base, base + GROUP):
                if target == 0:
                    portion[c] = out_buf[m, 0, rows_of(j)]
                else:
                    hand(c, target).start()

    def pair(c):
        m, j = c // per_micro, lax.rem(c, per_micro)

        @pl.when(section > 0)
        def _():
            with jax.named_scope("handed"):
                hand(c, 0).wait_recv()

        for f in range(features):
            group, part = f // lane_groups, f % lane_groups
            piece = portion[c, :, group * 128 : (group + 1) * 128].astype(jnp.float32)
            if part:
                piece = pltpu.roll(piece, 128 - part * features, 1)
            square[pl.ds(f, PIECE, stride=features), :] = piece
        whole = square[...].reshape(PIECE, features, 128)[:, :, :features]
        both = (whole + jnp.swapaxes(whole, 1, 2)).astype(jnp.bfloat16)
        pairs[...] = lax.dot_general(
            both, emb[m, rows_of(j)], (((2,), (1,)), ((0,), (0,))),
            preferred_element_type=jnp.float32,
        ).reshape(PIECE * features, width)
        def rows_for(f):
            return pairs[pl.ds(f, PIECE, stride=features), :].astype(jnp.bfloat16)

        for target in range(owners):
            for slot in range(direct):
                f = (target * slots + slot) // row_split
                outgoing[target, c, :, slot * width : (slot + 1) * width] = rows_for(f)
        opposite = [(target + half) % owners for target in range(owners)]
        for target in range(owners):
            for slot in range(kept):
                f = (target * slots + direct + slot) // row_split
                made = rows_for(f)
                extra_out[target, c, :, slot * width : (slot + 1) * width] = made
                lane = (kept + slot) * width
                extra_out[opposite[target], c, :, lane : lane + width] = made

        def send_far(k, carry):
            exchange(c, lax.rem(neighbour(k) + half, owners)).start()
            return carry

        def send_close(k, carry):
            exchange(c, neighbour(k)).start()
            if kept:
                exchange_near(c, neighbour(k)).start()
            return carry

        lax.fori_loop(0, half, send_far, 0)
        lax.fori_loop(1, half, send_close, 0)
        pltpu.make_async_copy(outgoing.at[owner, c], landing(c), recv_sem.at[c]).start()
        if kept:
            pltpu.make_async_copy(extra_out.at[owner, c], near_landing(c), close_sem.at[c]).start()

    def weigh(m):
        def product():
            return lax.dot_general(
                inp[m], slope[m].reshape(sections * quarter, hidden), (((0,), (0,)), ((), ())),
                preferred_element_type=jnp.float32,
            )

        @pl.when(m == 0)
        def _():
            load_inp().wait()
            acc[...] = product()

        @pl.when(m > 0)
        def _():
            acc[...] += product()

    def block_of(d):
        at = exclusive_or(owner, d, bits) * block
        return pl.ds(pl.multiple_of(at, block), block)

    def send_block(d, k, count):
        wsend[d, :, :count] = acc[block_of(d), :count].astype(jnp.bfloat16)
        reduce_copy(d, k, count).start()

    def reduce_stage(k, part=None, full=False):
        held = owners >> k
        top = held // 2 if part == 1 else held
        count = held if part is None else held // 2

        def across(stage):
            return hidden if full or stage == 0 else main

        def one(i, carry):
            h = top - 1 - i
            if k > 0:
                d = (1 << (k - 1)) + h * (1 << k)
                come = across(k - 1)
                reduce_copy(d, k - 1, come).wait_recv()
                at = block_of(h * (1 << k))
                acc[at, :come] = acc[at, :come] + wrecv[d, :, :come].astype(jnp.float32)
            if k < bits:
                ahead = h >= held // 2 if k == 1 and not full else True
                @pl.when((lax.rem(h, 2) == 1) & ahead)
                def _():
                    send_block(h * (1 << k), k, across(k))
            if k == 1 and not full:
                @pl.when(h > 0)
                def _():
                    side_send[h] = acc[block_of(h * 2), main:].astype(jnp.bfloat16)
                    side_copy(h).start()

            return carry

        with jax.named_scope(f"reduce{k}"):
            lax.fori_loop(0, count, one, 0)

    def send_rest():
        with jax.named_scope("rest"):
            for h in range(1, half // 2, 2):
                send_block(2 * h, 1, main)

    def side_sum(source):
        with jax.named_scope("side"):
            total = jnp.zeros((block, hidden - main), jnp.float32)
            for h in range(1, half):
                landed = side_recv.at[source, h]
                pltpu.make_async_copy(landed, landed, side_in.at[source, h]).wait()
                total = total + side_recv[source, h].astype(jnp.float32)
            sum_send[source] = total.astype(jnp.bfloat16)
            sum_copy(source).start()

    def send_ids():
        load_raw().wait()
        for target in range(owners):
            for slot in range(slots):
                f = (target * slots + slot) // row_split
                mine[target, :, slot : slot + 1, :] = raw[:, f : f + 1, :]
        pltpu.make_async_copy(mine.at[owner], places.at[owner], ids_recv).start()

        def send(k, carry):
            exchange_ids(lax.rem(owner + k, owners)).start()
            return carry

        lax.fori_loop(1, owners, send, 0)
        if kept:
            own = near_places.at[owner - base_owner]
            pltpu.make_async_copy(mine.at[mirror], own, near_recv).start()

            def send_near(k, carry):
                near_ids_copy(neighbour(k)).start()
                return carry

            lax.fori_loop(1, half, send_near, 0)

    def gather_ids():
        pltpu.make_async_copy(places, places, ids_recv).wait()
        for m in range(micro_count):
            for source in range(owners):
                ids[m, :, source * quarter : (source + 1) * quarter] = places[
                    source, m
                ]
        tacc[...] = jnp.zeros_like(tacc)
        if kept:
            pltpu.make_async_copy(near_places, near_places, near_recv).wait()
            for m in range(micro_count):
                for source in range(half):
                    near_ids[m, :, source * quarter : (source + 1) * quarter] = near_places[
                        source, m
                    ]
            nacc[...] = jnp.zeros_like(nacc)

    def collect(total, which, sources, first, rows, here, home, base=None):
        span = min(SPAN, sources * quarter)
        step = span // quarter

        def one(b, carry):
            at = first * quarter + b * span
            start = first if base is None else base
            block_rows = rows[0][rows[1], pl.ds(start + b * step, step)]
            block_rows = block_rows.reshape(span, block_rows.shape[-1])
            for slot, target, lane in which:
                row_block = lax.rem(home * slots + slot, row_split)
                named = here[0][here[1], slot : slot + 1, pl.ds(pl.multiple_of(at, span), span)]
                positions = lax.broadcasted_iota(jnp.int32, (TROWS, span), 0)
                onehot = (positions == named - row_block * TROWS).astype(jnp.float32)
                total[target] += lax.dot_general(
                    onehot.astype(jnp.bfloat16),
                    block_rows[:, lane * width : (lane + 1) * width],
                    (((1,), (0,)), ((), ())), preferred_element_type=jnp.float32,
                )
            return carry

        lax.fori_loop(0, sources * quarter // span, one, 0)

    def tabulate(m):
        for j in range(per_micro):
            batch = arrived.at[m, :, pl.ds(j * PIECE, PIECE)]
            pltpu.make_async_copy(batch, batch, recv_sem.at[m * per_micro + j]).wait()
            if kept:
                batch = near.at[m, :, pl.ds(j * PIECE, PIECE)]
                pltpu.make_async_copy(batch, batch, close_sem.at[m * per_micro + j]).wait()
        with jax.named_scope("tabulate"):
            everyone = [(slot, slot, slot) for slot in range(direct)]
            collect(tacc, everyone, owners, 0, (arrived, m), (ids, m), owner)
            if kept:
                close = [(direct + i, direct + i, i) for i in range(kept)]
                collect(tacc, close, half, base_owner, (near, m), (ids, m), owner, 0)
                other = [(direct + i, i, kept + i) for i in range(kept)]
                collect(nacc, other, half, 0, (near, m), (near_ids, m), mirror)

    def share_tables():
        for target in range(sections):
            @pl.when(section != target)
            def _():
                tsend[target] = tacc[:, target * share : (target + 1) * share, :].astype(jnp.bfloat16)
                share_copy(target).start()

            if kept:
                nsend[target] = nacc[:, target * share : (target + 1) * share, :].astype(jnp.bfloat16)
                near_share(target).start()

    with jax.named_scope("entry"):
        pl.semaphore_wait(barrier, owners - 1 + (sections - 1) * (2 if kept else 1))

    @pl.when(section == last)
    def _():
        for target in range(last):
            pl.semaphore_signal(
                ready, inc=1, device_id={"section": target},
                device_id_type=pl.DeviceIdType.MESH,
            )

    load_w().wait()

    @pl.when(section == last)
    def _():
        def first(m, carry):
            with jax.named_scope("head"):
                head(m)
            return carry

        def second(m, carry):
            with jax.named_scope("weigh"):
                weigh(m)
            return carry

        lax.fori_loop(0, micro_count, first, 0)
        lax.fori_loop(0, micro_count, second, 0)
        reduce_stage(0, None, True)
        send_ids()
        reduce_stage(1, None, True)

    @pl.when(section < last)
    def _():
        with jax.named_scope("turn"):
            wt[...] = w[...].T
        send_ids()
        for m in range(micro_count):
            load_pre(m).wait()
        pl.semaphore_wait(ready, 1)

    lag = jnp.where((section == last) | (section == 0), 0, section * 2 + 1)
    most = last * 2 - 1

    def step(t, carry):
        @pl.when((section < last) & (t < chunks))
        def _():
            for i in range(subs):
                with jax.named_scope("chain"):
                    chain(t, i)

            @pl.when(lax.rem(t, per_micro) == per_micro - 1)
            def _():
                with jax.named_scope("weigh"):
                    weigh(t // per_micro)

            @pl.when(t == chunks - 1)
            def _():
                reduce_stage(0)

        p = t - lag

        @pl.when((p >= 0) & (p < chunks))
        def _():
            @pl.when(p == 0)
            def _():
                load_emb().wait()

            with jax.named_scope("pair"):
                pair(p)

        @pl.when((section < last) & (t == chunks))
        def _():
            reduce_stage(1)

        for k in range(2, bits + 1):
            @pl.when((section == last) & (t == 5 * (k - 1)))
            def _():
                reduce_stage(k, None, True)

        @pl.when(p == per_micro)
        def _():
            with jax.named_scope("ids"):
                gather_ids()

        @pl.when((p >= 2 * per_micro) & (lax.rem(p, per_micro) == 0) & (p < chunks))
        def _():
            tabulate(p // per_micro - 2)

        return carry

    rounds = jnp.where(section == 0, chunks + 1, chunks + max(most, 5 * bits - chunks, 1))
    lax.fori_loop(0, rounds, step, 0)

    @pl.when((section > 0) & (section < last))
    def _():
        reduce_stage(2, 0)

    tabulate(micro_count - 2)
    tabulate(micro_count - 1)
    share_tables()

    @pl.when(section == last)
    def _():
        for source in range(last - 1, -1, -1):
            side_sum(source)

    @pl.when(section < last)
    def _():
        send_rest()

    @pl.when(section == 0)
    def _():
        reduce_stage(2, 0)

    def drain_chain(u, carry):
        along(u).wait_send()
        return carry

    @pl.when(section > 0)
    def _():
        lax.fori_loop(0, chunks * subs, drain_chain, 0)

    def drain_hand(c, carry):
        sent = out_buf.at[c // per_micro, pl.ds(0, last), rows_of(lax.rem(c, per_micro))]
        pltpu.make_async_copy(sent, sent, hand_sem.at[c]).wait()
        return carry

    @pl.when(section == 0)
    def _():
        lax.fori_loop(0, chunks, drain_hand, 0)

    def drain_far(k, carry):
        target = lax.rem(neighbour(k) + half, owners)
        sent = outgoing.at[target]
        pltpu.make_async_copy(sent, sent, send_sem.at[target]).wait()
        return carry

    def drain_close(k, carry):
        target = neighbour(k)
        sent = outgoing.at[target]
        pltpu.make_async_copy(sent, sent, send_sem.at[target]).wait()
        if kept:
            sent = extra_out.at[target]
            pltpu.make_async_copy(sent, sent, near_send.at[target]).wait()
            near_ids_copy(target).wait_send()
        return carry

    lax.fori_loop(0, half, drain_far, 0)
    lax.fori_loop(1, half, drain_close, 0)

    @pl.when(section < last)
    def _():
        reduce_stage(2, 1)
        for k in range(3, bits + 1):
            reduce_stage(k)
        with jax.named_scope("sum"):
            pltpu.make_async_copy(sum_recv, sum_recv, sum_in).wait()
            acc[block_of(0), main:] = acc[block_of(0), main:] + sum_recv[...].astype(jnp.float32)

    wg_ref[...] = acc[block_of(0), :]

    here = pl.ds(pl.multiple_of(section * share, share), share)
    total = tacc[:, here, :]
    with jax.named_scope("shared"):
        for k in range(1, sections):
            source = lax.rem(section + k, sections)
            pltpu.make_async_copy(trecv.at[source], trecv.at[source], trecv_sem.at[source]).wait()
            total = total + trecv[source].astype(jnp.float32)
        table_ref[...] = total
        if kept:
            extra = jnp.zeros((kept, share, width), jnp.float32)
            for source in range(sections):
                pltpu.make_async_copy(nrecv.at[source], nrecv.at[source], nrecv_sem.at[source]).wait()
                extra = extra + nrecv[source].astype(jnp.float32)
            table_ref[direct:slots] = table_ref[direct:slots] + extra

    def drain_owner(k, carry):
        exchange_ids(lax.rem(owner + k, owners)).wait_send()
        return carry

    lax.fori_loop(1, owners, drain_owner, 0)


    def drain_blocks(full):
        for k in range(bits):
            for h in range(owners >> (k + 1)):
                count = hidden if full or k == 0 else main
                reduce_copy((1 << k) + h * (2 << k), k, count).wait_send()

    @pl.when(section == last)
    def _():
        drain_blocks(True)
        for target in range(last):
            sum_copy(target).wait_send()

    @pl.when(section < last)
    def _():
        drain_blocks(False)
        for h in range(1, half):
            side_copy(h).wait_send()

    if kept:
        for target in range(sections):
            near_share(target).wait_send()
    for k in range(1, sections):
        share_copy(lax.rem(section + k, sections)).wait_send()


def scale_kernel(grad_scale, wg_ref, table_ref, wg_out, table_out):
    wg_out[...] = wg_ref[...] * grad_scale
    table_out[...] = table_ref[...] * grad_scale


def whole_step(layer_w, layer_pre, cotangent, layer_in, embeddings, row_ids, slots, row_split):
    sections = lax.axis_size("section")
    owners = lax.axis_size("owner")
    micro_count, batch_rows, hidden = cotangent.shape
    quarter, features, width = embeddings.shape[1:]
    chunks = micro_count * (quarter // PIECE)
    share = TROWS // sections
    direct = slots - slots // PROXY
    block, aside = hidden // owners, hidden // SIDE // 128 * 128
    kept = max(1, slots // PROXY)
    dims = (sections, owners, micro_count, quarter, features, width, slots, row_split)
    vmem = pl.BlockSpec(memory_space=pltpu.VMEM)
    anywhere = pl.BlockSpec(memory_space=pltpu.HBM)
    narrow, wide, whole = jnp.bfloat16, jnp.float32, jnp.int32
    split = (micro_count, sections, quarter, hidden)
    dma = pltpu.SemaphoreType.DMA
    return pl.pallas_call(
        functools.partial(step_kernel, dims),
        out_shape=(
            jax.ShapeDtypeStruct((hidden // owners, hidden), wide),
            jax.ShapeDtypeStruct((slots, share, width), wide),
        ),
        in_specs=[anywhere] * 6,
        out_specs=(vmem, vmem),
        scratch_shapes=[
            pltpu.VMEM((hidden, hidden), narrow),
            pltpu.VMEM((hidden, hidden), narrow),
            pltpu.VMEM(split, narrow),
            pltpu.VMEM(split, narrow),
            pltpu.VMEM((micro_count, batch_rows, hidden), narrow),
            pltpu.VMEM(embeddings.shape, narrow),
            pltpu.VMEM((micro_count, features, quarter), whole),
            pltpu.VMEM(split, narrow),
            pltpu.VMEM(split, narrow),
            pltpu.VMEM(split, narrow),
            pltpu.VMEM((chunks, PIECE, hidden), narrow),
            pltpu.VMEM((PIECE * features, 128), wide),
            pltpu.VMEM((PIECE * features, width), wide),
            pltpu.VMEM((owners, chunks, PIECE, direct * width), narrow),
            pltpu.VMEM((owners, chunks, PIECE, 2 * kept * width), narrow),
            pltpu.VMEM((micro_count, owners, quarter, direct * width), narrow),
            pltpu.VMEM((micro_count, owners // 2, quarter, 2 * kept * width), narrow),
            pltpu.VMEM((owners, micro_count, slots, quarter), whole),
            pltpu.VMEM((owners, micro_count, slots, quarter), whole),
            pltpu.VMEM((owners // 2, micro_count, slots, quarter), whole),
            pltpu.VMEM((micro_count, slots, owners * quarter), whole),
            pltpu.VMEM((micro_count, slots, owners * quarter // 2), whole),
            pltpu.VMEM((hidden, hidden), wide),
            pltpu.VMEM((owners, hidden // owners, hidden), narrow),
            pltpu.VMEM((owners, hidden // owners, hidden), narrow),
            pltpu.VMEM((slots, TROWS, width), wide),
            pltpu.VMEM((kept, TROWS, width), wide),
            pltpu.VMEM((sections, slots, share, width), narrow),
            pltpu.VMEM((sections, slots, share, width), narrow),
            pltpu.VMEM((sections, kept, share, width), narrow),
            pltpu.VMEM((sections, kept, share, width), narrow),
            pltpu.VMEM((owners // 2, block, aside), narrow),
            pltpu.VMEM((sections - 1, owners // 2, block, aside), narrow),
            pltpu.VMEM((sections - 1, block, aside), narrow),
            pltpu.VMEM((block, aside), narrow),
            dma(()),
            dma((micro_count,)),
            dma((micro_count,)),
            dma(()),
            dma(()),
            dma(()),
            dma((chunks * sections // GROUP,)),
            dma((chunks * sections // GROUP,)),
            dma((chunks,)),
            dma((chunks,)),
            dma((owners,)),
            dma((chunks,)),
            dma((chunks,)),
            dma((owners,)),
            dma(()),
            dma((owners,)),
            dma((owners,)),
            dma(()),
            dma((owners,)),
            dma((owners,)),
            dma((sections,)),
            dma((sections,)),
            dma((sections,)),
            dma((sections,)),
            dma((owners // 2,)),
            dma((sections - 1, owners // 2)),
            dma((sections - 1,)),
            dma(()),
            pltpu.SemaphoreType.REGULAR,
        ],
        compiler_params=pltpu.CompilerParams(
            collective_id=0, has_side_effects=True, vmem_limit_bytes=54272 * 1024
        ),
    )(
        layer_w, layer_pre.reshape(split), cotangent.reshape(split), layer_in, embeddings,
        pltpu.with_memory_space_constraint(jnp.swapaxes(row_ids, 1, 2), pltpu.HBM),
    )


def per_device(weights, inputs, preact, cotangent, embeddings, row_ids):
    owners = lax.axis_size("owner")
    micro_count, batch_rows, hidden = cotangent.shape
    features = embeddings.shape[2]
    row_split = max(1, owners // features)
    slots = features * row_split // owners
    grad_scale = 1.0 / math.sqrt(micro_count * batch_rows * owners)
    weight_grad, table_grad = whole_step(
        weights[0], preact[0], cotangent, inputs[0], embeddings, row_ids, slots, row_split
    )
    vmem = pl.BlockSpec(memory_space=pltpu.VMEM)
    weight_grad, table_grad = pl.pallas_call(
        functools.partial(scale_kernel, grad_scale),
        out_shape=(
            jax.ShapeDtypeStruct(weight_grad.shape, jnp.float32),
            jax.ShapeDtypeStruct(table_grad.shape, jnp.float32),
        ),
        in_specs=[vmem, vmem],
        out_specs=(vmem, vmem),
        compiler_params=pltpu.CompilerParams(vmem_limit_bytes=8 * 1024 * 1024),
    )(weight_grad, table_grad)
    return (weight_grad[None], table_grad)


def solution(mesh):
    return jax.shard_map(
        per_device,
        mesh=mesh,
        in_specs=(
            P("section", None, None),
            P("section", None, "owner", None),
            P("section", None, "owner", None),
            P(None, "owner", None),
            P(None, ("owner", "section"), None, None),
            P(None, ("owner", "section"), None),
        ),
        out_specs=(P("section", "owner", None), P("owner", "section", None)),
        check_vma=False,
    )
```

```python
import functools
import math

import jax
import jax.numpy as jnp
from jax import lax
from jax.experimental import pallas as pl
from jax.experimental.pallas import tpu as pltpu
from jax.sharding import PartitionSpec as P

TROWS = 512
PIECE = 16
SPAN = 512
GROUP = 2
PROXY = 4
SIDE = 4


def exclusive_or(a, b, bits):
    total = 0
    for k in range(bits):
        total = total + lax.rem(a // (1 << k) + b // (1 << k), 2) * (1 << k)
    return total


def step_kernel(
    dims, w_hbm, pre_hbm, cot_hbm, in_hbm, emb_hbm, ids_hbm, wg_ref, table_ref,
    w, wt, pre, cot, inp, emb, raw, slope, in_buf, out_buf, portion, square, pairs, outgoing,
    extra_out,
    arrived, near, mine, places, near_places, ids, near_ids, acc, wsend, wrecv, tacc, nacc,
    tsend, trecv, nsend, nrecv, side_send, side_recv, sum_send, sum_recv,
    w_sem, pre_sem, cot_sem, inp_sem, emb_sem, raw_sem, out_sem, in_sem, hand_sem, portion_sem,
    send_sem, recv_sem, close_sem, ids_send, ids_recv, near_send, near_ids_send, near_recv, wsend_sem, wrecv_sem,
    tsend_sem, trecv_sem, nsend_sem, nrecv_sem, side_out, side_in, sum_out, sum_in, ready,
):
    sections, owners, micro_count, quarter, features, width, slots, row_split = dims
    section = lax.axis_index("section")
    owner = lax.axis_index("owner")
    last = sections - 1
    lane_groups = 128 // features
    hidden = w.shape[0]
    per_micro = quarter // PIECE
    chunks = micro_count * per_micro
    subs = sections // GROUP
    bits = owners.bit_length() - 1
    block = hidden // owners
    share = TROWS // sections
    half = owners // 2
    kept = slots // PROXY
    direct = slots - kept
    main = hidden - hidden // SIDE // 128 * 128
    base_owner = owner // half * half
    mirror = lax.rem(owner + half, owners)

    barrier = pltpu.get_barrier_semaphore()
    for k in range(1, sections):
        pl.semaphore_signal(
            barrier, inc=1, device_id={"section": lax.rem(section + k, sections)},
            device_id_type=pl.DeviceIdType.MESH,
        )
    for k in range(1, owners):
        pl.semaphore_signal(
            barrier, inc=1, device_id={"owner": lax.rem(owner + k, owners)},
            device_id_type=pl.DeviceIdType.MESH,
        )

    if kept:
        for k in range(1, sections):
            pl.semaphore_signal(
                barrier, inc=1,
                device_id={"section": lax.rem(section + k, sections), "owner": mirror},
                device_id_type=pl.DeviceIdType.MESH,
            )

    def load_w():
        return pltpu.make_async_copy(w_hbm, w, w_sem)

    def load_pre(m):
        return pltpu.make_async_copy(pre_hbm.at[m], pre.at[m], pre_sem.at[m])

    def load_cot(m):
        return pltpu.make_async_copy(cot_hbm.at[m], cot.at[m], cot_sem.at[m])

    def load_inp():
        return pltpu.make_async_copy(in_hbm, inp, inp_sem)

    def load_emb():
        return pltpu.make_async_copy(emb_hbm, emb, emb_sem)

    def load_raw():
        return pltpu.make_async_copy(ids_hbm, raw, raw_sem)

    load_w().start()
    for m in range(micro_count):
        load_pre(m).start()

        @pl.when(section == last)
        def _():
            load_cot(m).start()

    load_raw().start()
    load_emb().start()
    load_inp().start()

    def rows_of(j):
        return pl.ds(pl.multiple_of(j * PIECE, PIECE), PIECE)

    def place(u):
        c = u // subs
        base = (subs - 1 - lax.rem(u, subs)) * GROUP
        return c // per_micro, pl.ds(base, GROUP), rows_of(lax.rem(c, per_micro))

    def along(u):
        at = place(u)
        return pltpu.make_async_remote_copy(
            src_ref=out_buf.at[at], dst_ref=in_buf.at[at],
            send_sem=out_sem.at[u], recv_sem=in_sem.at[u],
            device_id={"section": lax.rem(section + last, sections)},
            device_id_type=pl.DeviceIdType.MESH,
        )

    def hand(c, target):
        return pltpu.make_async_remote_copy(
            src_ref=out_buf.at[c // per_micro, target, rows_of(lax.rem(c, per_micro))],
            dst_ref=portion.at[c],
            send_sem=hand_sem.at[c], recv_sem=portion_sem.at[c],
            device_id={"section": target},
            device_id_type=pl.DeviceIdType.MESH,
        )

    def landing(c):
        return arrived.at[c // per_micro, owner, rows_of(lax.rem(c, per_micro))]

    def near_landing(c):
        return near.at[c // per_micro, owner - base_owner, rows_of(lax.rem(c, per_micro))]

    def exchange(c, target):
        return pltpu.make_async_remote_copy(
            src_ref=outgoing.at[target, c], dst_ref=landing(c),
            send_sem=send_sem.at[target], recv_sem=recv_sem.at[c],
            device_id={"owner": target},
            device_id_type=pl.DeviceIdType.MESH,
        )

    def exchange_near(c, target):
        return pltpu.make_async_remote_copy(
            src_ref=extra_out.at[target, c], dst_ref=near_landing(c),
            send_sem=near_send.at[target], recv_sem=close_sem.at[c],
            device_id={"owner": target},
            device_id_type=pl.DeviceIdType.MESH,
        )

    def exchange_ids(target):
        return pltpu.make_async_remote_copy(
            src_ref=mine.at[target], dst_ref=places.at[owner],
            send_sem=ids_send.at[target], recv_sem=ids_recv,
            device_id={"owner": target},
            device_id_type=pl.DeviceIdType.MESH,
        )

    def near_ids_copy(target):
        return pltpu.make_async_remote_copy(
            src_ref=mine.at[lax.rem(target + half, owners)],
            dst_ref=near_places.at[owner - base_owner],
            send_sem=near_ids_send.at[target], recv_sem=near_recv,
            device_id={"owner": target},
            device_id_type=pl.DeviceIdType.MESH,
        )

    def reduce_copy(d, k, count):
        across = pl.ds(0, count)
        return pltpu.make_async_remote_copy(
            src_ref=wsend.at[d, :, across], dst_ref=wrecv.at[d, :, across],
            send_sem=wsend_sem.at[d], recv_sem=wrecv_sem.at[d],
            device_id={"owner": exclusive_or(owner, 1 << k, bits)},
            device_id_type=pl.DeviceIdType.MESH,
        )

    def side_copy(h):
        return pltpu.make_async_remote_copy(
            src_ref=side_send.at[h], dst_ref=side_recv.at[section, h],
            send_sem=side_out.at[h], recv_sem=side_in.at[section, h],
            device_id={"section": last, "owner": exclusive_or(owner, 2 * h, bits)},
            device_id_type=pl.DeviceIdType.MESH,
        )

    def sum_copy(target):
        return pltpu.make_async_remote_copy(
            src_ref=sum_send.at[target], dst_ref=sum_recv,
            send_sem=sum_out.at[target], recv_sem=sum_in,
            device_id={"section": target},
            device_id_type=pl.DeviceIdType.MESH,
        )

    def share_copy(target):
        return pltpu.make_async_remote_copy(
            src_ref=tsend.at[target], dst_ref=trecv.at[section],
            send_sem=tsend_sem.at[target], recv_sem=trecv_sem.at[section],
            device_id={"section": target},
            device_id_type=pl.DeviceIdType.MESH,
        )

    def near_share(target):
        return pltpu.make_async_remote_copy(
            src_ref=nsend.at[target], dst_ref=nrecv.at[section],
            send_sem=nsend_sem.at[target], recv_sem=nrecv_sem.at[section],
            device_id={"section": target, "owner": mirror},
            device_id_type=pl.DeviceIdType.MESH,
        )

    def neighbour(k):
        return base_owner + lax.rem(owner - base_owner + k, half)

    def head(m):
        load_pre(m).wait()
        load_cot(m).wait()
        positive = pre[m].astype(jnp.float32) > 0
        slope[m] = jnp.where(positive, cot[m].astype(jnp.float32), 0.0).astype(jnp.bfloat16)
        out_buf[m] = lax.dot_general(
            slope[m].reshape(sections * quarter, hidden), w[...], (((1,), (1,)), ((), ())),
            preferred_element_type=jnp.float32,
        ).astype(jnp.bfloat16).reshape(sections, quarter, hidden)

    def head_send(m):
        def send(i, carry):
            along(m * per_micro * subs + i).start()
            return carry

        lax.fori_loop(0, per_micro * subs, send, 0)

    def chain(c, i):
        u = c * subs + i
        m, j = c // per_micro, lax.rem(c, per_micro)
        base = (subs - 1 - i) * GROUP
        at = (m, pl.ds(base, GROUP), rows_of(j))
        positive = pre[at].astype(jnp.float32) > 0
        with jax.named_scope("arrive"):
            along(u).wait_recv()
        grad = in_buf[at].astype(jnp.float32)
        slope[at] = jnp.where(positive, grad, 0.0).astype(jnp.bfloat16)
        out_buf[at] = lax.dot_general(
            slope[at].reshape(GROUP * PIECE, hidden), wt[...], (((1,), (0,)), ((), ())),
            preferred_element_type=jnp.float32,
        ).astype(jnp.bfloat16).reshape(GROUP, PIECE, hidden)

        @pl.when(section > 0)
        def _():
            along(u).start()

        @pl.when(section == 0)
        def _():
            for target in range(base, base + GROUP):
                if target == 0:
                    portion[c] = out_buf[m, 0, rows_of(j)]
                else:
                    hand(c, target).start()

    def pair(c):
        m, j = c // per_micro, lax.rem(c, per_micro)

        @pl.when(section > 0)
        def _():
            with jax.named_scope("handed"):
                hand(c, 0).wait_recv()

        for f in range(features):
            group, part = f // lane_groups, f % lane_groups
            piece = portion[c, :, group * 128 : (group + 1) * 128].astype(jnp.float32)
            if part:
                piece = pltpu.roll(piece, 128 - part * features, 1)
            square[pl.ds(f, PIECE, stride=features), :] = piece
        whole = square[...].reshape(PIECE, features, 128)[:, :, :features]
        both = (whole + jnp.swapaxes(whole, 1, 2)).astype(jnp.bfloat16)
        pairs[...] = lax.dot_general(
            both, emb[m, rows_of(j)], (((2,), (1,)), ((0,), (0,))),
            preferred_element_type=jnp.float32,
        ).reshape(PIECE * features, width)
        def rows_for(f):
            return pairs[pl.ds(f, PIECE, stride=features), :].astype(jnp.bfloat16)

        for target in range(owners):
            for slot in range(direct):
                f = (target * slots + slot) // row_split
                outgoing[target, c, :, slot * width : (slot + 1) * width] = rows_for(f)
        opposite = [(target + half) % owners for target in range(owners)]
        for target in range(owners):
            for slot in range(kept):
                f = (target * slots + direct + slot) // row_split
                made = rows_for(f)
                extra_out[target, c, :, slot * width : (slot + 1) * width] = made
                lane = (kept + slot) * width
                extra_out[opposite[target], c, :, lane : lane + width] = made

        def send_far(k, carry):
            exchange(c, lax.rem(neighbour(k) + half, owners)).start()
            return carry

        def send_close(k, carry):
            exchange(c, neighbour(k)).start()
            if kept:
                exchange_near(c, neighbour(k)).start()
            return carry

        lax.fori_loop(0, half, send_far, 0)
        lax.fori_loop(1, half, send_close, 0)
        pltpu.make_async_copy(outgoing.at[owner, c], landing(c), recv_sem.at[c]).start()
        if kept:
            pltpu.make_async_copy(extra_out.at[owner, c], near_landing(c), close_sem.at[c]).start()

    def weigh(m):
        def product():
            return lax.dot_general(
                inp[m], slope[m].reshape(sections * quarter, hidden), (((0,), (0,)), ((), ())),
                preferred_element_type=jnp.float32,
            )

        @pl.when(m == 0)
        def _():
            load_inp().wait()
            acc[...] = product()

        @pl.when(m > 0)
        def _():
            acc[...] += product()

    def block_of(d):
        at = exclusive_or(owner, d, bits) * block
        return pl.ds(pl.multiple_of(at, block), block)

    def send_block(d, k, count):
        wsend[d, :, :count] = acc[block_of(d), :count].astype(jnp.bfloat16)
        reduce_copy(d, k, count).start()

    def reduce_stage(k, part=None, full=False):
        held = owners >> k
        top = held // 2 if part == 1 else held
        count = held if part is None else held // 2

        def across(stage):
            return hidden if full or stage == 0 else main

        def one(i, carry):
            h = top - 1 - i
            if k > 0:
                d = (1 << (k - 1)) + h * (1 << k)
                come = across(k - 1)
                reduce_copy(d, k - 1, come).wait_recv()
                at = block_of(h * (1 << k))
                acc[at, :come] = acc[at, :come] + wrecv[d, :, :come].astype(jnp.float32)
            if k < bits:
                ahead = h >= held // 2 if k == 1 and not full else True
                @pl.when((lax.rem(h, 2) == 1) & ahead)
                def _():
                    send_block(h * (1 << k), k, across(k))
            if k == 1 and not full:
                @pl.when(h > 0)
                def _():
                    side_send[h] = acc[block_of(h * 2), main:].astype(jnp.bfloat16)
                    side_copy(h).start()

            return carry

        with jax.named_scope(f"reduce{k}"):
            lax.fori_loop(0, count, one, 0)

    def send_rest():
        with jax.named_scope("rest"):
            for h in range(1, half // 2, 2):
                send_block(2 * h, 1, main)

    def side_sum(source):
        with jax.named_scope("side"):
            total = jnp.zeros((block, hidden - main), jnp.float32)
            for h in range(1, half):
                landed = side_recv.at[source, h]
                pltpu.make_async_copy(landed, landed, side_in.at[source, h]).wait()
                total = total + side_recv[source, h].astype(jnp.float32)
            sum_send[source] = total.astype(jnp.bfloat16)
            sum_copy(source).start()

    def send_ids():
        load_raw().wait()
        for target in range(owners):
            for slot in range(slots):
                f = (target * slots + slot) // row_split
                mine[target, :, slot : slot + 1, :] = raw[:, f : f + 1, :]
        pltpu.make_async_copy(mine.at[owner], places.at[owner], ids_recv).start()

        def send(k, carry):
            exchange_ids(lax.rem(owner + k, owners)).start()
            return carry

        lax.fori_loop(1, owners, send, 0)
        if kept:
            own = near_places.at[owner - base_owner]
            pltpu.make_async_copy(mine.at[mirror], own, near_recv).start()

            def send_near(k, carry):
                near_ids_copy(neighbour(k)).start()
                return carry

            lax.fori_loop(1, half, send_near, 0)

    def gather_ids():
        pltpu.make_async_copy(places, places, ids_recv).wait()
        for m in range(micro_count):
            for source in range(owners):
                ids[m, :, source * quarter : (source + 1) * quarter] = places[
                    source, m
                ]
        tacc[...] = jnp.zeros_like(tacc)
        if kept:
            pltpu.make_async_copy(near_places, near_places, near_recv).wait()
            for m in range(micro_count):
                for source in range(half):
                    near_ids[m, :, source * quarter : (source + 1) * quarter] = near_places[
                        source, m
                    ]
            nacc[...] = jnp.zeros_like(nacc)

    def collect(total, which, sources, first, rows, here, home, base=None):
        span = min(SPAN, sources * quarter)
        step = span // quarter

        def one(b, carry):
            at = first * quarter + b * span
            start = first if base is None else base
            block_rows = rows[0][rows[1], pl.ds(start + b * step, step)]
            block_rows = block_rows.reshape(span, block_rows.shape[-1])
            for slot, target, lane in which:
                row_block = lax.rem(home * slots + slot, row_split)
                named = here[0][here[1], slot : slot + 1, pl.ds(pl.multiple_of(at, span), span)]
                positions = lax.broadcasted_iota(jnp.int32, (TROWS, span), 0)
                onehot = (positions == named - row_block * TROWS).astype(jnp.float32)
                total[target] += lax.dot_general(
                    onehot.astype(jnp.bfloat16),
                    block_rows[:, lane * width : (lane + 1) * width],
                    (((1,), (0,)), ((), ())), preferred_element_type=jnp.float32,
                )
            return carry

        lax.fori_loop(0, sources * quarter // span, one, 0)

    def tabulate(m):
        for j in range(per_micro):
            batch = arrived.at[m, :, pl.ds(j * PIECE, PIECE)]
            pltpu.make_async_copy(batch, batch, recv_sem.at[m * per_micro + j]).wait()
            if kept:
                batch = near.at[m, :, pl.ds(j * PIECE, PIECE)]
                pltpu.make_async_copy(batch, batch, close_sem.at[m * per_micro + j]).wait()
        with jax.named_scope("tabulate"):
            everyone = [(slot, slot, slot) for slot in range(direct)]
            collect(tacc, everyone, owners, 0, (arrived, m), (ids, m), owner)
            if kept:
                close = [(direct + i, direct + i, i) for i in range(kept)]
                collect(tacc, close, half, base_owner, (near, m), (ids, m), owner, 0)
                other = [(direct + i, i, kept + i) for i in range(kept)]
                collect(nacc, other, half, 0, (near, m), (near_ids, m), mirror)

    def share_tables():
        for target in range(sections):
            @pl.when(section != target)
            def _():
                tsend[target] = tacc[:, target * share : (target + 1) * share, :].astype(jnp.bfloat16)
                share_copy(target).start()

            if kept:
                nsend[target] = nacc[:, target * share : (target + 1) * share, :].astype(jnp.bfloat16)
                near_share(target).start()

    @pl.when(section == last)
    def _():
        load_w().wait()
        head(0)

    with jax.named_scope("entry"):
        pl.semaphore_wait(barrier, owners - 1 + (sections - 1) * (2 if kept else 1))

    @pl.when(section == last)
    def _():
        for target in range(last):
            pl.semaphore_signal(
                ready, inc=1, device_id={"section": target},
                device_id_type=pl.DeviceIdType.MESH,
            )

    @pl.when(section == last)
    def _():
        head_send(0)

        def first(m, carry):
            with jax.named_scope("head"):
                head(m)
                head_send(m)
            return carry

        def second(m, carry):
            with jax.named_scope("weigh"):
                weigh(m)
            return carry

        lax.fori_loop(1, micro_count, first, 0)
        lax.fori_loop(0, micro_count, second, 0)
        reduce_stage(0, None, True)
        send_ids()
        reduce_stage(1, None, True)

    @pl.when(section < last)
    def _():
        load_w().wait()
        with jax.named_scope("turn"):
            wt[...] = w[...].T
        send_ids()
        for m in range(micro_count):
            load_pre(m).wait()
        pl.semaphore_wait(ready, 1)

    lag = jnp.where((section == last) | (section == 0), 0, section * 2 + 1)
    most = last * 2 - 1

    def step(t, carry):
        @pl.when((section < last) & (t < chunks))
        def _():
            for i in range(subs):
                with jax.named_scope("chain"):
                    chain(t, i)

            @pl.when(lax.rem(t, per_micro) == per_micro - 1)
            def _():
                with jax.named_scope("weigh"):
                    weigh(t // per_micro)

            @pl.when(t == chunks - 1)
            def _():
                reduce_stage(0)

        p = t - lag

        @pl.when((p >= 0) & (p < chunks))
        def _():
            @pl.when(p == 0)
            def _():
                load_emb().wait()

            with jax.named_scope("pair"):
                pair(p)

        @pl.when((section < last) & (t == chunks))
        def _():
            reduce_stage(1)

        for k in range(2, bits + 1):
            @pl.when((section == last) & (t == 5 * (k - 1)))
            def _():
                reduce_stage(k, None, True)

        @pl.when(p == per_micro)
        def _():
            with jax.named_scope("ids"):
                gather_ids()

        @pl.when((p >= 2 * per_micro) & (lax.rem(p, per_micro) == 0) & (p < chunks))
        def _():
            tabulate(p // per_micro - 2)

        return carry

    rounds = jnp.where(section == 0, chunks + 1, chunks + max(most, 5 * bits - chunks, 1))
    lax.fori_loop(0, rounds, step, 0)

    @pl.when((section > 0) & (section < last))
    def _():
        reduce_stage(2, 0)

    tabulate(micro_count - 2)
    tabulate(micro_count - 1)
    share_tables()

    @pl.when(section == last)
    def _():
        for source in range(last - 1, -1, -1):
            side_sum(source)

    @pl.when(section < last)
    def _():
        send_rest()

    @pl.when(section == 0)
    def _():
        reduce_stage(2, 0)

    def drain_chain(u, carry):
        along(u).wait_send()
        return carry

    @pl.when(section > 0)
    def _():
        lax.fori_loop(0, chunks * subs, drain_chain, 0)

    def drain_hand(c, carry):
        sent = out_buf.at[c // per_micro, pl.ds(0, last), rows_of(lax.rem(c, per_micro))]
        pltpu.make_async_copy(sent, sent, hand_sem.at[c]).wait()
        return carry

    @pl.when(section == 0)
    def _():
        lax.fori_loop(0, chunks, drain_hand, 0)

    def drain_far(k, carry):
        target = lax.rem(neighbour(k) + half, owners)
        sent = outgoing.at[target]
        pltpu.make_async_copy(sent, sent, send_sem.at[target]).wait()
        return carry

    def drain_close(k, carry):
        target = neighbour(k)
        sent = outgoing.at[target]
        pltpu.make_async_copy(sent, sent, send_sem.at[target]).wait()
        if kept:
            sent = extra_out.at[target]
            pltpu.make_async_copy(sent, sent, near_send.at[target]).wait()
            near_ids_copy(target).wait_send()
        return carry

    lax.fori_loop(0, half, drain_far, 0)
    lax.fori_loop(1, half, drain_close, 0)

    @pl.when(section < last)
    def _():
        reduce_stage(2, 1)
        for k in range(3, bits + 1):
            reduce_stage(k)
        with jax.named_scope("sum"):
            pltpu.make_async_copy(sum_recv, sum_recv, sum_in).wait()
            acc[block_of(0), main:] = acc[block_of(0), main:] + sum_recv[...].astype(jnp.float32)

    wg_ref[...] = acc[block_of(0), :]

    here = pl.ds(pl.multiple_of(section * share, share), share)
    total = tacc[:, here, :]
    with jax.named_scope("shared"):
        for k in range(1, sections):
            source = lax.rem(section + k, sections)
            pltpu.make_async_copy(trecv.at[source], trecv.at[source], trecv_sem.at[source]).wait()
            total = total + trecv[source].astype(jnp.float32)
        table_ref[...] = total
        if kept:
            extra = jnp.zeros((kept, share, width), jnp.float32)
            for source in range(sections):
                pltpu.make_async_copy(nrecv.at[source], nrecv.at[source], nrecv_sem.at[source]).wait()
                extra = extra + nrecv[source].astype(jnp.float32)
            table_ref[direct:slots] = table_ref[direct:slots] + extra

    def drain_owner(k, carry):
        exchange_ids(lax.rem(owner + k, owners)).wait_send()
        return carry

    lax.fori_loop(1, owners, drain_owner, 0)


    def drain_blocks(full):
        for k in range(bits):
            for h in range(owners >> (k + 1)):
                count = hidden if full or k == 0 else main
                reduce_copy((1 << k) + h * (2 << k), k, count).wait_send()

    @pl.when(section == last)
    def _():
        drain_blocks(True)
        for target in range(last):
            sum_copy(target).wait_send()

    @pl.when(section < last)
    def _():
        drain_blocks(False)
        for h in range(1, half):
            side_copy(h).wait_send()

    if kept:
        for target in range(sections):
            near_share(target).wait_send()
    for k in range(1, sections):
        share_copy(lax.rem(section + k, sections)).wait_send()


def scale_kernel(grad_scale, wg_ref, table_ref, wg_out, table_out):
    wg_out[...] = wg_ref[...] * grad_scale
    table_out[...] = table_ref[...] * grad_scale


def whole_step(layer_w, layer_pre, cotangent, layer_in, embeddings, row_ids, slots, row_split):
    sections = lax.axis_size("section")
    owners = lax.axis_size("owner")
    micro_count, batch_rows, hidden = cotangent.shape
    quarter, features, width = embeddings.shape[1:]
    chunks = micro_count * (quarter // PIECE)
    share = TROWS // sections
    direct = slots - slots // PROXY
    block, aside = hidden // owners, hidden // SIDE // 128 * 128
    kept = max(1, slots // PROXY)
    dims = (sections, owners, micro_count, quarter, features, width, slots, row_split)
    vmem = pl.BlockSpec(memory_space=pltpu.VMEM)
    anywhere = pl.BlockSpec(memory_space=pltpu.HBM)
    narrow, wide, whole = jnp.bfloat16, jnp.float32, jnp.int32
    split = (micro_count, sections, quarter, hidden)
    dma = pltpu.SemaphoreType.DMA
    return pl.pallas_call(
        functools.partial(step_kernel, dims),
        out_shape=(
            jax.ShapeDtypeStruct((hidden // owners, hidden), wide),
            jax.ShapeDtypeStruct((slots, share, width), wide),
        ),
        in_specs=[anywhere] * 6,
        out_specs=(vmem, vmem),
        scratch_shapes=[
            pltpu.VMEM((hidden, hidden), narrow),
            pltpu.VMEM((hidden, hidden), narrow),
            pltpu.VMEM(split, narrow),
            pltpu.VMEM(split, narrow),
            pltpu.VMEM((micro_count, batch_rows, hidden), narrow),
            pltpu.VMEM(embeddings.shape, narrow),
            pltpu.VMEM((micro_count, features, quarter), whole),
            pltpu.VMEM(split, narrow),
            pltpu.VMEM(split, narrow),
            pltpu.VMEM(split, narrow),
            pltpu.VMEM((chunks, PIECE, hidden), narrow),
            pltpu.VMEM((PIECE * features, 128), wide),
            pltpu.VMEM((PIECE * features, width), wide),
            pltpu.VMEM((owners, chunks, PIECE, direct * width), narrow),
            pltpu.VMEM((owners, chunks, PIECE, 2 * kept * width), narrow),
            pltpu.VMEM((micro_count, owners, quarter, direct * width), narrow),
            pltpu.VMEM((micro_count, owners // 2, quarter, 2 * kept * width), narrow),
            pltpu.VMEM((owners, micro_count, slots, quarter), whole),
            pltpu.VMEM((owners, micro_count, slots, quarter), whole),
            pltpu.VMEM((owners // 2, micro_count, slots, quarter), whole),
            pltpu.VMEM((micro_count, slots, owners * quarter), whole),
            pltpu.VMEM((micro_count, slots, owners * quarter // 2), whole),
            pltpu.VMEM((hidden, hidden), wide),
            pltpu.VMEM((owners, hidden // owners, hidden), narrow),
            pltpu.VMEM((owners, hidden // owners, hidden), narrow),
            pltpu.VMEM((slots, TROWS, width), wide),
            pltpu.VMEM((kept, TROWS, width), wide),
            pltpu.VMEM((sections, slots, share, width), narrow),
            pltpu.VMEM((sections, slots, share, width), narrow),
            pltpu.VMEM((sections, kept, share, width), narrow),
            pltpu.VMEM((sections, kept, share, width), narrow),
            pltpu.VMEM((owners // 2, block, aside), narrow),
            pltpu.VMEM((sections - 1, owners // 2, block, aside), narrow),
            pltpu.VMEM((sections - 1, block, aside), narrow),
            pltpu.VMEM((block, aside), narrow),
            dma(()),
            dma((micro_count,)),
            dma((micro_count,)),
            dma(()),
            dma(()),
            dma(()),
            dma((chunks * sections // GROUP,)),
            dma((chunks * sections // GROUP,)),
            dma((chunks,)),
            dma((chunks,)),
            dma((owners,)),
            dma((chunks,)),
            dma((chunks,)),
            dma((owners,)),
            dma(()),
            dma((owners,)),
            dma((owners,)),
            dma(()),
            dma((owners,)),
            dma((owners,)),
            dma((sections,)),
            dma((sections,)),
            dma((sections,)),
            dma((sections,)),
            dma((owners // 2,)),
            dma((sections - 1, owners // 2)),
            dma((sections - 1,)),
            dma(()),
            pltpu.SemaphoreType.REGULAR,
        ],
        compiler_params=pltpu.CompilerParams(
            collective_id=0, has_side_effects=True, vmem_limit_bytes=54272 * 1024
        ),
    )(
        layer_w, layer_pre.reshape(split), cotangent.reshape(split), layer_in, embeddings,
        pltpu.with_memory_space_constraint(jnp.swapaxes(row_ids, 1, 2), pltpu.HBM),
    )


def per_device(weights, inputs, preact, cotangent, embeddings, row_ids):
    owners = lax.axis_size("owner")
    micro_count, batch_rows, hidden = cotangent.shape
    features = embeddings.shape[2]
    row_split = max(1, owners // features)
    slots = features * row_split // owners
    grad_scale = 1.0 / math.sqrt(micro_count * batch_rows * owners)
    weight_grad, table_grad = whole_step(
        weights[0], preact[0], cotangent, inputs[0], embeddings, row_ids, slots, row_split
    )
    vmem = pl.BlockSpec(memory_space=pltpu.VMEM)
    weight_grad, table_grad = pl.pallas_call(
        functools.partial(scale_kernel, grad_scale),
        out_shape=(
            jax.ShapeDtypeStruct(weight_grad.shape, jnp.float32),
            jax.ShapeDtypeStruct(table_grad.shape, jnp.float32),
        ),
        in_specs=[vmem, vmem],
        out_specs=(vmem, vmem),
        compiler_params=pltpu.CompilerParams(vmem_limit_bytes=8 * 1024 * 1024),
    )(weight_grad, table_grad)
    return (weight_grad[None], table_grad)


def solution(mesh):
    return jax.shard_map(
        per_device,
        mesh=mesh,
        in_specs=(
            P("section", None, None),
            P("section", None, "owner", None),
            P("section", None, "owner", None),
            P(None, "owner", None),
            P(None, ("owner", "section"), None, None),
            P(None, ("owner", "section"), None),
        ),
        out_specs=(P("section", "owner", None), P("owner", "section", None)),
        check_vma=False,
    )
```
